32 devices in a mesh: gx: 4 (over y, x), gy: 2 (over core), gz: 4 (over z).
Axes of the slice: x: 2, y: 2, z: 4, core: 2. Of those that a mesh axis runs over, the one named last changes fastest.
Arguments:
- positions: float32 [3, 4, 8, 16, 64], P(None, 'gz', 'gx', 'gy'), may hold values from 0 to 1
- counts: int32 [4, 8, 16], P('gz', 'gx', 'gy'), may hold values from 16 to 64, as said below
Outputs:
- force: float32 [3, 4, 8, 16, 64], P(None, 'gz', 'gx', 'gy')
- energy: float32 [4, 8, 16, 64], P('gz', 'gx', 'gy')
The draws below stay inside these ranges and needn't reach their ends.
Inputs may be any that keep to these rules, and one draw needn't show every extreme that they name: `counts`: every draw has some full cells.
All inputs are finite; a program needn't handle non-finite values.
Results may differ from the reference program's by a relative error of at most 0.0003.
Values sent between devices are 32-bit elements; how exact they have to be, the bound alone decides.
A program may use at most 64 MiB of HBM per device.

```python
import jax
import jax.numpy as jnp
from jax import lax

SLOTS = 64
NX = 8
NY = 16
NZ = 4


def draw_counts(key, part):
    first = jax.random.fold_in(key, 11)
    second = jax.random.fold_in(key, 23)
    base = jax.random.randint(first, (NZ, NX, NY), SLOTS // 4, 3 * SLOTS // 4 + 1)
    full = jax.random.randint(second, (NZ, NX, NY), 0, 16) == 0
    counts = jnp.where(full, SLOTS, base)
    counts = counts.at[0, 0, 0].set(SLOTS)
    return counts.astype(jnp.int32)


def block_levels(rng, extent, shards, least, largest):
    loudness, own = 1.0, jax.random.fold_in(rng, 6)
    for position, blocks in shards:
        draws = jnp.exp(jax.random.uniform(jax.random.fold_in(own, position), (blocks,), jnp.float32, least / len(shards), largest / len(shards)))
        loudness = loudness * jnp.repeat(draws, extent[position] // blocks).reshape([-1 if axis == position else 1 for axis in range(len(extent))])
    return loudness


def setup_inputs(seed: int = 0) -> dict:
    keys = jax.random.split(jax.random.key(seed), 3)
    return {
        "positions": jnp.clip(1.0 * jax.random.uniform(keys[0], (3, NZ, NX, NY, SLOTS), jnp.float32) ** block_levels(keys[0], (3, NZ, NX, NY, SLOTS), ((1, 4), (2, 4), (3, 2)), -0.2, 0.2), 0.0, 1.0),
        "counts": draw_counts(jax.random.fold_in(keys[2], 71), 0),
    }


cutoff_sq = 4.95 * 4.95
cell_sides = (12.0, 12.0, 2.5)
density_width = 8.0
pair_width = 3.0
density_amp = 1.0
pair_amp = 2.0

def kernels(squared):
    inside = jnp.where(squared < cutoff_sq, 1.0 - squared / cutoff_sq, 0.0)
    smooth = inside * inside
    smooth_slope = -2.0 * inside / cutoff_sq
    first = jnp.exp(-squared / density_width)
    second = jnp.exp(-squared / pair_width)
    return (density_amp * first * smooth, density_amp * first * (smooth_slope - smooth / density_width), pair_amp * second * smooth, pair_amp * second * (smooth_slope - smooth / pair_width))

def neighbours(extended, centre_z, start_x, start_y, rows_x, rows_y, step_z, step_x):
    pieces = []
    for step_y in (-1, 0, 1):
        pieces.append(extended[:, centre_z + step_z, start_x + step_x:start_x + step_x + rows_x, start_y + step_y:start_y + step_y + rows_y])
    return jnp.concatenate(pieces, axis=-1)

def pair_geometry(center, partner, step_z, step_x, slots):
    lateral = (jnp.arange(3 * slots) // slots - 1).astype(jnp.float32)
    moves = (float(step_x), lateral, float(step_z))
    squared = jnp.zeros((), jnp.float32)
    deltas = []
    for component in range(3):
        delta = (center[component][..., :, None] - partner[component][..., None, :] - moves[component]) * cell_sides[component]
        deltas.append(delta)
        squared = squared + delta * delta
    weight = center[3][..., :, None] * partner[3][..., None, :]
    if step_z == 0 and step_x == 0:
        column = jnp.arange(3 * slots)[None, :]
        row_index = jnp.arange(slots)[:, None]
        weight = weight * (column != row_index + slots).astype(jnp.float32)
    return (deltas, squared, weight)

def densities(extended, centre_z, start_x, start_y, rows_x, rows_y, slots):
    center = extended[:, centre_z, start_x:start_x + rows_x, start_y:start_y + rows_y]
    summed = jnp.zeros(center.shape[1:], jnp.float32)
    for step_z in range(-2, 3):
        for step_x in range(-1, 2):
            partner = neighbours(extended, centre_z, start_x, start_y, rows_x, rows_y, step_z, step_x)
            deltas, squared, weight = pair_geometry(center, partner, step_z, step_x, slots)
            summed = summed + lax.optimization_barrier(jnp.sum(weight * kernels(squared)[0], axis=-1))
    return summed

def forces(extended, centre_z, rows_x, rows_y, slots):
    center = extended[:, centre_z, 1:1 + rows_x, 1:1 + rows_y]
    pushes = [jnp.zeros(center.shape[1:], jnp.float32) for component in range(3)]
    pairs = jnp.zeros(center.shape[1:], jnp.float32)
    for step_z in range(-2, 3):
        for step_x in range(-1, 2):
            partner = neighbours(extended, centre_z, 1, 1, rows_x, rows_y, step_z, step_x)
            deltas, squared, weight = pair_geometry(center, partner, step_z, step_x, slots)
            values = kernels(squared)
            factor = weight * ((center[4][..., :, None] + partner[4][..., None, :]) * values[1] + values[3])
            pushes = [pushes[component] - 2.0 * lax.optimization_barrier(jnp.sum(factor * deltas[component], axis=-1)) for component in range(3)]
            pairs = pairs + lax.optimization_barrier(jnp.sum(weight * values[2], axis=-1))
    return (jnp.stack(pushes), pairs)

def reference(positions, counts):
    occupied = (jnp.arange(SLOTS)[None, None, None, :] < counts[..., None]).astype(jnp.float32)
    stacked = jnp.concatenate([positions, occupied[None]], axis=0)

    def window(source, layer):
        layers = ((layer + jnp.arange(-2, 3)) % NZ).astype(jnp.int32)
        taken = jnp.take(source, layers, axis=1)
        return jnp.pad(taken, ((0, 0), (0, 0), (1, 1), (1, 1), (0, 0)), mode='wrap')

    def first_pass(layer):
        return densities(window(stacked, layer), 2, 1, 1, NX, NY, SLOTS)
    density = lax.map(first_pass, jnp.arange(NZ))
    root = jnp.sqrt(1.0 + density)
    slope = -0.5 / root
    full = jnp.concatenate([stacked, slope[None]], axis=0)

    def second_pass(layer):
        return forces(window(full, layer), 2, NX, NY, SLOTS)
    pushes, pairs = lax.map(second_pass, jnp.arange(NZ))
    force = jnp.moveaxis(pushes, 0, 1)
    energy = occupied * (-root + 0.5 * pairs)
    return (force, energy)
```

```python
import functools
import math

import jax
import jax.numpy as jnp
from jax import lax
from jax.experimental import pallas as pl
from jax.experimental.pallas import tpu as pltpu
from jax.sharding import PartitionSpec as P

CUT = 4.95
SIDES = (12.0, 12.0, 2.5)
FAR = 1024.0
LOG2E = math.log2(math.e)
SCALE = math.sqrt(LOG2E / 8.0)
REACH = CUT * CUT * LOG2E / 8.0
SPLIT = 0.5
SLIDES = tuple(side * SCALE for side in SIDES)
A = 2.0 * LOG2E
B = 0.75 * LOG2E
G1 = 2.0 ** (-REACH) / REACH**2
G2 = 2.0 ** (-REACH * 8.0 / 3.0) / REACH**2
SIGMA = (3.0 / 16.0) * G1 / G2
CLASSES = 4
SUB = 8
STATIC = 8
VMEM_BYTES = 67_043_328
SPARE = 16384
DEPTH = 2
LAYERS = 2 * DEPTH + 1
VMEM = pl.BlockSpec(memory_space=pltpu.VMEM)
HBM = pl.BlockSpec(memory_space=pltpu.HBM)


AXES = ("gz", "gx", "gy")


def layer_slots(nz):
    kept = []
    for a in range(-DEPTH, DEPTH + 1):
        if all((a - k) % nz for k in kept):
            kept.append(a)
    slot = [
        next(i for i, k in enumerate(kept) if (a - k) % nz == 0)
        for a in range(-DEPTH, DEPTH + 1)
    ]
    return kept, slot


def displacements(sizes):
    kept, _ = layer_slots(sizes[0])
    copies, others = [], []
    for s, a in enumerate(kept):
        for b in (-1, 0, 1):
            for c in (-1, 0, 1):
                if (a, b, c) == (0, 0, 0):
                    continue
                step = tuple(-o % n for o, n in zip((a, b, c), sizes))
                copies.append((s, b, c, step))
                if any(step) and step not in others:
                    others.append(step)
    return copies, others


def device(step, sizes):
    return {
        axis: lax.rem(lax.axis_index(axis) + d, n)
        for axis, d, n in zip(AXES, step, sizes)
    }


def enter(sizes):
    _, others = displacements(sizes)
    barrier = pltpu.get_barrier_semaphore()
    for step in others:
        pl.semaphore_signal(
            barrier,
            inc=1,
            device_id=device(step, sizes),
            device_id_type=pl.DeviceIdType.MESH,
        )
    return barrier, len(others)


def edge(offset, length):
    if offset == 0:
        return pl.ds(0, length), pl.ds(1, length)
    if offset < 0:
        return pl.ds(length - 1, 1), pl.ds(0, 1)
    return pl.ds(0, 1), pl.ds(length + 1, 1)


def link(sizes, rx, nt, own, ext, send, recv, s, b, c, step):
    (sx, dx), (st, dt) = edge(b, rx), edge(c, nt)
    source, target = own.at[sx, st], ext.at[s, dx, dt]
    j = 3 * (b + 1) + c + 1
    if not any(step):
        return pltpu.make_async_copy(source, target, recv.at[s, j])
    return pltpu.make_async_remote_copy(
        src_ref=source,
        dst_ref=target,
        send_sem=send.at[s, j],
        recv_sem=recv.at[s, j],
        device_id=device(step, sizes),
        device_id_type=pl.DeviceIdType.MESH,
    )


def start_copies(sizes, rx, nt, own, ext, send, recv):
    copies, _ = displacements(sizes)
    started = []
    for s, b, c, step in copies:
        copy = link(sizes, rx, nt, own, ext, send, recv, s, b, c, step)
        copy.start()
        if any(step):
            started.append(copy)
    return started


def wait_layer(sizes, rx, nt, own, ext, send, recv, slot, a):
    for b in (-1, 0, 1):
        for c in (-1, 0, 1):
            if a is None:
                step = (1, 0, 0)
            else:
                if (a, b, c) == (0, 0, 0):
                    continue
                step = tuple(-o % n for o, n in zip((a, b, c), sizes))
            copy = link(sizes, rx, nt, own, ext, send, recv, slot, b, c, step)
            if any(step):
                copy.wait_recv()
            else:
                copy.wait()


def arrival_order(nz):
    _, slots = layer_slots(nz)
    if nz < 4:
        return [(slots[a + DEPTH], a, a + DEPTH, a) for a in (0, 1, -1, 2, -2)]
    near = jnp.where(lax.axis_index("gz") == nz - 1, -1, 1)
    return [
        (slots[DEPTH], 0, DEPTH, 0),
        (near + DEPTH, near, near + DEPTH, None),
        (slots[0], -2, 0, -2),
        (slots[2 * DEPTH], 2, 2 * DEPTH, 2),
        (DEPTH - near, -near, DEPTH - near, None),
    ]


def iota(shape, dim):
    return lax.broadcasted_iota(jnp.int32, shape, dim)


def group_count(half):
    return (half + CLASSES * (SUB - 1)) // SUB


def load_rows(rx, nt, half, home, count_ref, pos_ref, own, ext, raw):
    lane = iota((1, 2 * half), 1)
    for x in range(rx):
        for t in range(nt):
            n0, n1 = count_ref[0, x, 2 * t], count_ref[0, x, 2 * t + 1]
            occupied = jnp.where(lane < half, lane - n0, lane - half - n1) < 0
            for c in range(3):
                rows = [pos_ref[c, 0, x, 2 * t + k : 2 * t + k + 1, :] for k in (0, 1)]
                row = jnp.concatenate(rows, axis=1)
                raw[c, pl.ds(x * nt + t, 1)] = jnp.where(occupied, row, FAR)
                row = jnp.where(occupied, row * SLIDES[c], FAR)
                own[x, t, c] = row
                ext[home, x + 1, t + 1, c] = row


def assign_slots(tiles, half, raw, slot_ref, cent_row, packed):
    width = 2 * half
    u, v, w = raw[0], raw[1], raw[2]
    here = u < 0.5 * FAR
    xhi, yhi = u >= SPLIT, v >= SPLIT
    masks = [
        here & ~xhi & ~yhi,
        here & ~xhi & yhi,
        here & xhi & ~yhi,
        here & xhi & yhi,
    ]
    ones = [jnp.where(m, 1.0, 0.0) for m in masks]
    i, j = iota((width, width), 0), iota((width, width), 1)
    same = i // half == j // half
    before = jnp.where(same & (i < j), 1.0, 0.0)
    whole = jnp.where(same, 1.0, 0.0)
    stacked = jnp.concatenate(ones, axis=0)
    ranks = jnp.dot(stacked, before, preferred_element_type=jnp.float32)
    totals = jnp.dot(stacked, whole, preferred_element_type=jnp.float32)
    upper = iota((tiles, width), 1) >= half
    slot = jnp.where(here, jnp.where(upper, float(width), 0.0), -2.0 * width)
    ends = jnp.zeros((tiles, width), jnp.float32)
    pack = jnp.zeros((tiles, width), jnp.float32)
    for k in range(CLASSES):
        rank, total = ranks[k * tiles : (k + 1) * tiles], totals[k * tiles : (k + 1) * tiles]
        slot = slot + ones[k] * (ends * SUB + rank)
        ends = ends + jnp.floor((total + (SUB - 1)) * (1.0 / SUB))
        pack = pack + ends * float(16**k)
    px = u * SLIDES[0] + jnp.where(xhi, 0.0, SLIDES[0])
    py = v * SLIDES[1] + jnp.where(yhi, 0.0, SLIDES[1])
    pz = w * SLIDES[2]
    for r in range(tiles):
        slot_ref[r] = slot[r : r + 1]
        packed[r] = pack[r : r + 1]
        for c, p in enumerate((px, py, pz)):
            cent_row[r, c] = p[r : r + 1]


def group_code(packed, r, k, half):
    lane = iota((1, 2 * half), 1)
    return jnp.sum(jnp.where(lane == k * half, packed[r], 0.0)).astype(jnp.int32)


def group_base(code, x, j, g, ry):
    b1, b2, b3 = code & 15, (code >> 4) & 15, (code >> 8) & 15
    xhi = jnp.where(b2 <= g, 1, 0)
    yhi = jnp.where(b3 <= g, 1, jnp.where(b2 <= g, 0, jnp.where(b1 <= g, 1, 0)))
    return (x + xhi) * (ry + 1) + j + yhi


def spread_centres(tiles, nt, ry, half, groups, stride, slot_ref, cent_row, packed, cen, meta):
    width = 2 * half
    sub = iota((SUB, width), 0).astype(jnp.float32)
    upper = jnp.where(iota((SUB, width), 1) >= half, SLIDES[1], 0.0)

    def step(r, carry):
        slot = slot_ref[r]
        rows = [cent_row[r, c] for c in range(3)]
        x, t = r // nt, r % nt
        for k in (0, 1):
            code = group_code(packed, r, k, half)
            for g in range(groups):
                i = (2 * r + k) * stride + g
                meta[i] = group_base(code, x, 2 * t + k, g, ry)
                pick = slot == sub + float(k * width + g * SUB)
                for c in range(3):
                    column = jnp.sum(jnp.where(pick, rows[c], 0.0), axis=1, keepdims=True)
                    wide = jnp.broadcast_to(column, (SUB, width))
                    if c == 1:
                        wide = wide - upper
                    cen[i, c] = wide
        return carry

    lax.fori_loop(0, tiles, step, 0)


def build_pairs(s, cols, ry, half, channels, ext, pairs):
    low = iota((1, 2 * half), 1) < half

    def step(x, carry):
        for c in range(channels):
            rows = [ext[s, x, t, c] for t in range(ry // 2 + 2)]
            for p in range(ry + 1):
                if p % 2:
                    row = rows[(p + 1) // 2]
                else:
                    row = pltpu.roll(jnp.where(low, rows[p // 2 + 1], rows[p // 2]), half, 1)
                pairs[s, x * (ry + 1) + p, c] = row
        return carry

    lax.fori_loop(0, cols, step, 0, unroll=2)


def density_layer(first, slot, shift, z, cells, groups, stride, ry, meta, pairs, cen, vs, rho):
    def step(cell, carry):
        for g in range(groups):
            i = cell * stride + g
            base = meta[i]
            x, y, w = cen[i, 0], cen[i, 1], cen[i, 2]
            if shift is not None:
                w = w - shift
            for b in (0, 1):
                qx, qy, qz = (pairs[slot, base + b * (ry + 1), c] for c in range(3))
                dx, dy, dz = x - qx, y - qy, w - qz
                v = jnp.maximum(((REACH - dx * dx) - dy * dy) - dz * dz, 0.0)
                vs[i, z, b] = v
                part = jnp.exp2(v) * (v * v)
                total = part if b == 0 else total + part
                x = x - SLIDES[0]
            rho[i] = total if first else rho[i] + total
        return carry

    lax.fori_loop(0, cells, step, 0, unroll=2)


def slope_pass(tiles, nt, half, groups, stride, slot_ref, rho, cs, root_ref, sown, sext, home):
    width = 2 * half
    sub = iota((SUB, width), 0).astype(jnp.float32)

    def step(r, carry):
        slot = slot_ref[r]
        value = jnp.zeros((SUB, width), jnp.float32)
        for k in (0, 1):
            for g in range(groups):
                i = (2 * r + k) * stride + g
                one_rho = jnp.sum(rho[i], axis=1, keepdims=True) * G1
                value = value + jnp.where(
                    slot == sub + float(k * width + g * SUB), one_rho, 0.0
                )
                one_rho = jnp.broadcast_to(one_rho, (SUB, width))
                cs[i] = (-0.5 * SIGMA) * lax.rsqrt(jnp.maximum(one_rho, 0.5))
        one_rho = jnp.sum(value, axis=0, keepdims=True)
        root = jnp.sqrt(jnp.where(slot >= 0.0, one_rho, 1.0))
        root_ref[r] = root
        row = (-0.5 * SIGMA) / root
        x, t = r // nt, r % nt
        sown[x, t, 0] = row
        sext[home, x + 1, t + 1, 0] = row
        return carry

    lax.fori_loop(0, tiles, step, 0)


def geometry(slots, ry, i, base, pairs, cen):
    x, y, w = cen[i, 0], cen[i, 1], cen[i, 2]
    for z in range(LAYERS):
        a = z - DEPTH
        wz = w - a * SLIDES[2] if a else w
        for b in (0, 1):
            q = [pairs[slots[z], base + b * (ry + 1), c] for c in range(3)]
            xb = x - SLIDES[0] if b else x
            yield z, b, (xb - q[0], y - q[1], wz - q[2])


def pair_terms(v):
    g = jnp.exp2(v) * ((v + A) * v)
    w = v * jnp.exp2(v * (8.0 / 3.0))
    return g, w * (v + B), w * v


def pair_pass(slots, cells, stride, ry, width, meta, pairs, cen, vs, gd, acc_ref):
    def step(cell, carry):
        for g in range(STATIC):
            i = cell * stride + g
            acc = [jnp.zeros((SUB, width), jnp.float32) for _ in range(4)]
            for z, b, d in geometry(slots, ry, i, meta[i], pairs, cen):
                dens, pair, phi = pair_terms(vs[i, z, b])
                for c in range(3):
                    gd[cell * STATIC + g, z, b, c] = dens * d[c]
                    acc[c] = acc[c] + pair * d[c]
                acc[3] = acc[3] + phi
            for c in range(4):
                acc_ref[i, c] = acc[c]
        return carry

    lax.fori_loop(0, cells, step, 0)


def slope_force(layers, cells, stride, ry, meta, spairs, cs, gd, acc_ref):
    def step(cell, carry):
        for g in range(STATIC):
            i = cell * stride + g
            base, sp = meta[i], cs[i]
            acc = [acc_ref[i, c] for c in range(3)]
            for slot, z in layers:
                for b in (0, 1):
                    f = sp + spairs[slot, base + b * (ry + 1), 0]
                    for c in range(3):
                        acc[c] = acc[c] + f * gd[cell * STATIC + g, z, b, c]
            for c in range(3):
                acc_ref[i, c] = acc[c]
        return carry

    lax.fori_loop(0, cells, step, 0)


def step_kernel(
    sizes, rx, nt, half, count_hbm, pos_hbm, slot_ref, packed, cen, pairs, vs, cs, root_ref,
    spairs, acc_ref, count_ref, pos_ref, own, ext, raw, cent_row, meta, rho, sown, sext, gd,
    load, send, recv, send2, recv2,
):
    loads = [
        pltpu.make_async_copy(count_hbm, count_ref, load.at[0]),
        pltpu.make_async_copy(pos_hbm, pos_ref, load.at[1]),
    ]
    for copy in loads:
        copy.start()
    barrier, arrivals = enter(sizes)
    ry, tiles, cells = 2 * nt, rx * nt, 2 * rx * nt
    width = 2 * half
    kept, slots = layer_slots(sizes[0])
    home = slots[DEPTH]
    groups = group_count(half)
    stride = group_stride(half)
    order = arrival_order(sizes[0])
    for copy in loads:
        copy.wait()
    load_rows(rx, nt, half, home, count_ref, pos_ref, own, ext, raw)
    pl.semaphore_wait(barrier, arrivals)
    sends = start_copies(sizes, rx, nt, own, ext, send, recv)
    assign_slots(tiles, half, raw, slot_ref, cent_row, packed)
    spread_centres(tiles, nt, ry, half, groups, stride, slot_ref, cent_row, packed, cen, meta)

    def arrive(e, own_ref, ext_ref, send_sem, recv_sem, channels, pairs_ref):
        slot, _, _, known = order[e]
        seen = [o[0] for o in order[:e] if isinstance(o[0], int)]
        if isinstance(slot, int) and slot in seen:
            return
        wait_layer(sizes, rx, nt, own_ref, ext_ref, send_sem, recv_sem, slot, known)
        build_pairs(slot, rx + 2, ry, half, channels, ext_ref, pairs_ref)

    for e, (slot, a, z, known) in enumerate(order):
        arrive(e, own, ext, send, recv, 3, pairs)
        if known is None:
            shift = a.astype(jnp.float32) * SLIDES[2]
        else:
            shift = known * SLIDES[2] if known else None
        density_layer(
            e == 0, slot, shift, z, cells, groups, stride, ry, meta, pairs, cen, vs, rho
        )
    slope_pass(tiles, nt, half, groups, stride, slot_ref, rho, cs, root_ref, sown, sext, home)
    sends += start_copies(sizes, rx, nt, sown, sext, send2, recv2)
    pair_pass(slots, cells, stride, ry, width, meta, pairs, cen, vs, gd, acc_ref)
    for chunk in ((0, 1), (2, 3), (4,)):
        for e in chunk:
            arrive(e, sown, sext, send2, recv2, 1, spairs)
        layers = [(order[e][0], order[e][2]) for e in chunk]
        slope_force(layers, cells, stride, ry, meta, spairs, cs, gd, acc_ref)
    for copy in sends:
        copy.wait_send()


def finish_kernel(
    slots, rx, nt, half, slot_ref, packed, cen, pairs, vs, cs, root_ref, spairs, acc_ref,
    force_ref, energy_ref, codes, values,
):
    width, ry, tiles = 2 * half, 2 * nt, rx * nt
    stride = group_stride(half)
    sub = iota((SUB, width), 0).astype(jnp.float32)
    for r in range(tiles):
        for k in (0, 1):
            codes[2 * r + k] = group_code(packed, r, k, half)

    def gather(r, carry):
        slot = slot_ref[r]
        total = [jnp.zeros((SUB, width), jnp.float32) for _ in range(4)]
        for k in (0, 1):
            for g in range(STATIC):
                pick = slot == sub + float(k * width + g * SUB)
                for c in range(4):
                    part = jnp.sum(acc_ref[(2 * r + k) * stride + g, c], axis=1, keepdims=True)
                    total[c] = total[c] + jnp.where(pick, part, 0.0)
        for c in range(4):
            values[r, c] = total[c]
        return carry

    lax.fori_loop(0, tiles, gather, 0, unroll=2)

    def rest(cell, carry):
        r, k = cell // 2, cell % 2
        x, j = r // nt, 2 * (r % nt) + k
        code = codes[cell]

        def group(g, carry):
            i = cell * stride + g
            base, sp = group_base(code, x, j, g, ry), cs[i]
            acc = [jnp.zeros((SUB, width), jnp.float32) for _ in range(4)]
            for z, b, d in geometry(slots, ry, i, base, pairs, cen):
                dens, pair, phi = pair_terms(vs[i, z, b])
                f = (sp + spairs[slots[z], base + b * (ry + 1), 0]) * dens + pair
                for c in range(3):
                    acc[c] = acc[c] + f * d[c]
                acc[3] = acc[3] + phi
            pick = slot_ref[r] == sub + (k * width + g * SUB).astype(jnp.float32)
            for c in range(4):
                part = jnp.sum(acc[c], axis=1, keepdims=True)
                values[r, c] = values[r, c] + jnp.where(pick, part, 0.0)
            return carry

        lax.fori_loop(STATIC, code >> 12, group, 0)
        return carry

    lax.fori_loop(0, 2 * tiles, rest, 0)

    for x in range(rx):
        for t in range(nt):
            r = x * nt + t
            for c in range(4):
                value = jnp.sum(values[r, c], axis=0, keepdims=True)
                if c < 3:
                    value = value * (4.0 / 3.0 * G2 / SCALE)
                else:
                    value = value * G2 - 1.0 - root_ref[r]
                value = jnp.where(slot_ref[r] >= 0.0, value, 0.0)
                for k in (0, 1):
                    part = value[:, k * half : (k + 1) * half]
                    if c < 3:
                        force_ref[c, 0, x, 2 * t + k : 2 * t + k + 1, :] = part
                    else:
                        energy_ref[0, x, 2 * t + k : 2 * t + k + 1, :] = part


def group_stride(half):
    return group_count(half)


def body(positions, counts):
    rx, ry, half = positions.shape[2:]
    nt, width = ry // 2, 2 * half
    f32 = jnp.float32
    sizes = tuple(lax.axis_size(axis) for axis in AXES)
    kept, slots = layer_slots(sizes[0])
    layers, tiles, cells = len(kept), rx * nt, rx * ry
    total = cells * group_stride(half)
    rows = (rx + 2) * (ry + 1)

    def vmem(*dims):
        return pltpu.VMEM(dims, f32)

    passed = (
            vmem(tiles, 1, width),
            vmem(tiles, 1, width),
            vmem(total, 3, SUB, width),
            vmem(layers, rows, 3, 1, width),
            vmem(total, LAYERS, 2, SUB, width),
            vmem(total, SUB, width),
            vmem(tiles, 1, width),
            vmem(layers, rows, 1, 1, width),
            vmem(total, 4, SUB, width),
    )
    held = sum(4 * math.prod(ref.shape) for ref in passed)
    shared = pl.pallas_call(
        functools.partial(step_kernel, sizes, rx, nt, half),
        out_shape=passed,
        in_specs=[HBM, HBM],
        out_specs=(VMEM,) * 9,
        scratch_shapes=[
            pltpu.SMEM(counts.shape, jnp.int32),
            vmem(*positions.shape),
            vmem(rx, nt, 3, 1, width),
            vmem(layers, rx + 2, nt + 2, 3, 1, width),
            vmem(3, tiles, width),
            vmem(tiles, 3, 1, width),
            pltpu.SMEM((total,), jnp.int32),
            vmem(total, SUB, width),
            vmem(rx, nt, 1, 1, width),
            vmem(layers, rx + 2, nt + 2, 1, 1, width),
            vmem(cells * STATIC, LAYERS, 2, 3, SUB, width),
            pltpu.SemaphoreType.DMA((2,)),
        ]
        + [pltpu.SemaphoreType.DMA((layers, 9))] * 4,
        compiler_params=pltpu.CompilerParams(
            collective_id=0, has_side_effects=True, vmem_limit_bytes=VMEM_BYTES - held - SPARE
        ),
        name="step",
    )(counts, positions)
    return pl.pallas_call(
        functools.partial(finish_kernel, slots, rx, nt, half),
        out_shape=(
            jax.ShapeDtypeStruct((3, 1, rx, ry, half), f32),
            jax.ShapeDtypeStruct((1, rx, ry, half), f32),
        ),
        in_specs=[VMEM] * 9,
        out_specs=(VMEM, VMEM),
        scratch_shapes=[pltpu.SMEM((cells,), jnp.int32), vmem(tiles, 4, SUB, width)],
        compiler_params=pltpu.CompilerParams(vmem_limit_bytes=24 * 2**20),
        name="finish",
    )(*shared)


def solution(mesh):
    return jax.shard_map(
        body,
        mesh=mesh,
        in_specs=(P(None, "gz", "gx", "gy", None), P("gz", "gx", "gy")),
        out_specs=(P(None, "gz", "gx", "gy", None), P("gz", "gx", "gy", None)),
        check_vma=False,
    )
```

```python
import functools
import math

import jax
import jax.numpy as jnp
from jax import lax
from jax.experimental import pallas as pl
from jax.experimental.pallas import tpu as pltpu
from jax.sharding import PartitionSpec as P

CUT = 4.95
SIDES = (12.0, 12.0, 2.5)
FAR = 1024.0
LOG2E = math.log2(math.e)
SCALE = math.sqrt(LOG2E / 8.0)
REACH = CUT * CUT * LOG2E / 8.0
SPLIT = 0.5
SLIDES = tuple(side * SCALE for side in SIDES)
A = 2.0 * LOG2E
B = 0.75 * LOG2E
G1 = 2.0 ** (-REACH) / REACH**2
G2 = 2.0 ** (-REACH * 8.0 / 3.0) / REACH**2
SIGMA = (3.0 / 16.0) * G1 / G2
CLASSES = 4
SUB = 8
STATIC = 8
VMEM_BYTES = 67_043_328
SPARE = 16384
DEPTH = 2
LAYERS = 2 * DEPTH + 1
VMEM = pl.BlockSpec(memory_space=pltpu.VMEM)
HBM = pl.BlockSpec(memory_space=pltpu.HBM)


AXES = ("gz", "gx", "gy")


def layer_slots(nz):
    kept = []
    for a in range(-DEPTH, DEPTH + 1):
        if all((a - k) % nz for k in kept):
            kept.append(a)
    slot = [
        next(i for i, k in enumerate(kept) if (a - k) % nz == 0)
        for a in range(-DEPTH, DEPTH + 1)
    ]
    return kept, slot


def displacements(sizes):
    kept, _ = layer_slots(sizes[0])
    copies, others = [], []
    for s, a in enumerate(kept):
        for b in (-1, 0, 1):
            for c in (-1, 0, 1):
                if (a, b, c) == (0, 0, 0):
                    continue
                step = tuple(-o % n for o, n in zip((a, b, c), sizes))
                copies.append((s, b, c, step))
                if any(step) and step not in others:
                    others.append(step)
    return copies, others


def device(step, sizes):
    return {
        axis: lax.rem(lax.axis_index(axis) + d, n)
        for axis, d, n in zip(AXES, step, sizes)
    }


def enter(sizes):
    _, others = displacements(sizes)
    barrier = pltpu.get_barrier_semaphore()
    for step in others:
        pl.semaphore_signal(
            barrier,
            inc=1,
            device_id=device(step, sizes),
            device_id_type=pl.DeviceIdType.MESH,
        )
    return barrier, len(others)


def edge(offset, length):
    if offset == 0:
        return pl.ds(0, length), pl.ds(1, length)
    if offset < 0:
        return pl.ds(length - 1, 1), pl.ds(0, 1)
    return pl.ds(0, 1), pl.ds(length + 1, 1)


def link(sizes, rx, nt, own, ext, send, recv, s, b, c, step):
    (sx, dx), (st, dt) = edge(b, rx), edge(c, nt)
    source, target = own.at[sx, st], ext.at[s, dx, dt]
    j = 3 * (b + 1) + c + 1
    if not any(step):
        return pltpu.make_async_copy(source, target, recv.at[s, j])
    return pltpu.make_async_remote_copy(
        src_ref=source,
        dst_ref=target,
        send_sem=send.at[s, j],
        recv_sem=recv.at[s, j],
        device_id=device(step, sizes),
        device_id_type=pl.DeviceIdType.MESH,
    )


def start_copies(sizes, rx, nt, own, ext, send, recv):
    copies, _ = displacements(sizes)
    started = []
    far = {s: abs(a) for s, a in enumerate(layer_slots(sizes[0])[0])}
    for s, b, c, step in sorted(copies, key=lambda copy: far[copy[0]]):
        copy = link(sizes, rx, nt, own, ext, send, recv, s, b, c, step)
        copy.start()
        if any(step):
            started.append(copy)
    return started


def wait_layer(sizes, rx, nt, own, ext, send, recv, slot, a, sides=(-1, 0, 1)):
    for b in sides:
        for c in (-1, 0, 1):
            if a is None:
                step = (1, 0, 0)
            else:
                if (a, b, c) == (0, 0, 0):
                    continue
                step = tuple(-o % n for o, n in zip((a, b, c), sizes))
            copy = link(sizes, rx, nt, own, ext, send, recv, slot, b, c, step)
            if any(step):
                copy.wait_recv()
            else:
                copy.wait()


def offsets_of(nz, slot):
    return [a for a in range(-DEPTH, DEPTH + 1) if layer_slots(nz)[1][a + DEPTH] == slot]


def arrival_order(nz):
    kept, slots = layer_slots(nz)
    home = slots[DEPTH]
    if nz < 4:
        rest = [s for s in range(len(kept)) if s != home]
        return [(s, kept[s], [(a, a + DEPTH) for a in offsets_of(nz, s)]) for s in [home] + rest]
    near = jnp.where(lax.axis_index("gz") == nz - 1, -1, 1)
    order = [(home, 0, [(0, DEPTH)]), (near + DEPTH, None, [(near, near + DEPTH)])]
    for s in sorted({slots[0], slots[2 * DEPTH]}):
        order.append((s, kept[s], [(a, a + DEPTH) for a in offsets_of(nz, s)]))
    order.append((DEPTH - near, None, [(-near, DEPTH - near)]))
    return order


def iota(shape, dim):
    return lax.broadcasted_iota(jnp.int32, shape, dim)


def group_count(half):
    return (half + CLASSES * (SUB - 1)) // SUB


def load_rows(rx, nt, half, home, count_ref, pos_ref, own, ext, raw):
    lane = iota((1, 2 * half), 1)
    for x in range(rx):
        for t in range(nt):
            n0, n1 = count_ref[0, x, 2 * t], count_ref[0, x, 2 * t + 1]
            occupied = jnp.where(lane < half, lane - n0, lane - half - n1) < 0
            for c in range(3):
                rows = [pos_ref[c, 0, x, 2 * t + k : 2 * t + k + 1, :] for k in (0, 1)]
                row = jnp.concatenate(rows, axis=1)
                raw[c, pl.ds(x * nt + t, 1)] = jnp.where(occupied, row, FAR)
                row = jnp.where(occupied, row * SLIDES[c], FAR)
                own[x, t, c] = row
                ext[home, x + 1, t + 1, c] = row


def assign_slots(tiles, half, raw, slot_ref, cent_row, packed):
    width = 2 * half
    u, v, w = raw[0], raw[1], raw[2]
    here = u < 0.5 * FAR
    xhi, yhi = u >= SPLIT, v >= SPLIT
    masks = [
        here & ~xhi & ~yhi,
        here & ~xhi & yhi,
        here & xhi & ~yhi,
        here & xhi & yhi,
    ]
    ones = [jnp.where(m, 1.0, 0.0) for m in masks]
    i, j = iota((width, width), 0), iota((width, width), 1)
    same = i // half == j // half
    before = jnp.where(same & (i < j), 1.0, 0.0)
    whole = jnp.where(same, 1.0, 0.0)
    stacked = jnp.concatenate(ones, axis=0)
    ranks = jnp.dot(stacked, before, preferred_element_type=jnp.float32)
    totals = jnp.dot(stacked, whole, preferred_element_type=jnp.float32)
    upper = iota((tiles, width), 1) >= half
    slot = jnp.where(here, jnp.where(upper, float(width), 0.0), -2.0 * width)
    ends = jnp.zeros((tiles, width), jnp.float32)
    pack = jnp.zeros((tiles, width), jnp.float32)
    for k in range(CLASSES):
        rank, total = ranks[k * tiles : (k + 1) * tiles], totals[k * tiles : (k + 1) * tiles]
        slot = slot + ones[k] * (ends * SUB + rank)
        ends = ends + jnp.floor((total + (SUB - 1)) * (1.0 / SUB))
        pack = pack + ends * float(16**k)
    px = u * SLIDES[0] + jnp.where(xhi, 0.0, SLIDES[0])
    py = v * SLIDES[1] + jnp.where(yhi, 0.0, SLIDES[1])
    pz = w * SLIDES[2]
    for r in range(tiles):
        slot_ref[r] = slot[r : r + 1]
        packed[r] = pack[r : r + 1]
        for c, p in enumerate((px, py, pz)):
            cent_row[r, c] = p[r : r + 1]


def group_code(packed, r, k, half):
    lane = iota((1, 2 * half), 1)
    return jnp.sum(jnp.where(lane == k * half, packed[r], 0.0)).astype(jnp.int32)


def group_place(code, g):
    b1, b2, b3 = code & 15, (code >> 4) & 15, (code >> 8) & 15
    xhi = jnp.where(b2 <= g, 1, 0)
    yhi = jnp.where(b3 <= g, 1, jnp.where(b2 <= g, 0, jnp.where(b1 <= g, 1, 0)))
    return xhi, yhi


def spread_centres(tiles, nt, ry, half, groups, stride, slot_ref, cent_row, packed, cen, meta):
    width = 2 * half
    sub = iota((SUB, width), 0).astype(jnp.float32)
    lean = jnp.where(iota((SUB, width), 1) >= half, 0.5 * SLIDES[1], -0.5 * SLIDES[1])

    def step(r, carry):
        slot = slot_ref[r]
        rows = [cent_row[r, c] for c in range(3)]
        x, t = r // nt, r % nt
        for k in (0, 1):
            code = group_code(packed, r, k, half)
            for g in range(groups):
                i = (2 * r + k) * stride + g
                xhi, yhi = group_place(code, g)
                meta[i] = (x + xhi) * (ry + 1) + 2 * t + k + yhi
                sign = jnp.where(yhi == k, -1.0, 1.0)
                pick = slot == sub + float(k * width + g * SUB)
                for c in range(3):
                    column = jnp.sum(jnp.where(pick, rows[c], 0.0), axis=1, keepdims=True)
                    wide = jnp.broadcast_to(column, (SUB, width))
                    if c == 1:
                        wide = wide - (0.5 * SLIDES[1] + sign * lean)
                    cen[i, c] = wide
        return carry

    lax.fori_loop(0, tiles, step, 0)


def build_pairs(s, first, last, ry, half, channels, ext, pairs):
    low = iota((1, 2 * half), 1) < half

    def step(x, carry):
        for c in range(channels):
            rows = [ext[s, x, t, c] for t in range(ry // 2 + 2)]
            for p in range(ry + 1):
                if p % 2:
                    row = rows[(p + 1) // 2]
                else:
                    row = jnp.where(low, rows[p // 2 + 1], rows[p // 2])
                pairs[s, x * (ry + 1) + p, c] = row
        return carry

    lax.fori_loop(first, last, step, 0, unroll=2 if (last - first) % 2 == 0 else 1)


def density_layer(
    sides, first, slot, offsets, rx, groups, stride, ry, meta, pairs, cen, vs, rho
):
    def run(x_cell):
        def step(j, carry):
            for g in range(groups):
                i = (x_cell * ry + j) * stride + g
                base = meta[i]
                x, y, w = cen[i, 0], cen[i, 1], cen[i, 2]
                ws = [w if shift is None else w - shift for shift, _ in offsets]
                total = None if first else rho[i]
                for b in sides[x_cell]:
                    qx, qy, qz = (pairs[slot, base + b * (ry + 1), c] for c in range(3))
                    dx, dy = (x - SLIDES[0] if b else x) - qx, y - qy
                    flat = (REACH - dx * dx) - dy * dy
                    for wz, (_, z) in zip(ws, offsets):
                        dz = wz - qz
                        v = jnp.maximum(flat - dz * dz, 0.0)
                        vs[i, z, b] = v
                        part = jnp.exp2(v) * (v * v)
                        total = part if total is None else total + part
                rho[i] = jnp.zeros_like(x) if total is None else total
            return carry

        return step

    for x_cell in range(rx):
        if sides[x_cell] or first:
            lax.fori_loop(0, ry, run(x_cell), 0, unroll=2)


def slope_pass(tiles, nt, half, groups, stride, slot_ref, rho, cs, root_ref, sown, sext, home):
    width = 2 * half
    sub = iota((SUB, width), 0).astype(jnp.float32)

    def step(r, carry):
        slot = slot_ref[r]
        value = jnp.zeros((SUB, width), jnp.float32)
        for k in (0, 1):
            for g in range(groups):
                i = (2 * r + k) * stride + g
                one_rho = jnp.sum(rho[i], axis=1, keepdims=True) * G1
                value = value + jnp.where(
                    slot == sub + float(k * width + g * SUB), one_rho, 0.0
                )
                one_rho = jnp.broadcast_to(one_rho, (SUB, width))
                cs[i] = (-0.5 * SIGMA) * lax.rsqrt(jnp.maximum(one_rho, 0.5))
        one_rho = jnp.sum(value, axis=0, keepdims=True)
        root = jnp.sqrt(jnp.where(slot >= 0.0, one_rho, 1.0))
        root_ref[r] = root
        row = (-0.5 * SIGMA) / root
        x, t = r // nt, r % nt
        sown[x, t, 0] = row
        sext[home, x + 1, t + 1, 0] = row
        return carry

    lax.fori_loop(0, tiles, step, 0, unroll=4)


def pair_terms(v):
    g = jnp.exp2(v) * ((v + A) * v)
    w = v * jnp.exp2(v * (8.0 / 3.0))
    return g, w * (v + B), w * v


def pair_sums(nz, ry, i, base, pairs, cen, vs):
    x, y, w = cen[i, 0], cen[i, 1], cen[i, 2]
    ws = [w - a * SLIDES[2] if a else w for a in range(-DEPTH, DEPTH + 1)]
    for slot in range(len(layer_slots(nz)[0])):
        for b in (0, 1):
            q = [pairs[slot, base + b * (ry + 1), c] for c in range(3)]
            dx, dy = (x - SLIDES[0] if b else x) - q[0], y - q[1]
            dens = pair = phi = dens_z = pair_z = 0.0
            for a in offsets_of(nz, slot):
                dz = ws[a + DEPTH] - q[2]
                d, p, f = pair_terms(vs[i, a + DEPTH, b])
                dens, pair, phi = dens + d, pair + p, phi + f
                dens_z, pair_z = dens_z + d * dz, pair_z + p * dz
            yield slot, b, (dens * dx, dens * dy, dens_z), (pair * dx, pair * dy, pair_z, phi)


def pair_pass(nz, cells, stride, ry, width, meta, pairs, cen, vs, gd, acc_ref):
    def step(cell, carry):
        for g in range(STATIC):
            i = cell * stride + g
            acc = [0.0] * 4
            for slot, b, dens, pair in pair_sums(nz, ry, i, meta[i], pairs, cen, vs):
                for c in range(3):
                    gd[cell * STATIC + g, slot, b, c] = dens[c]
                acc = [total + part for total, part in zip(acc, pair)]
            for c in range(4):
                acc_ref[i, c] = acc[c]
        return carry

    lax.fori_loop(0, cells, step, 0)


def slope_force(layers, cells, stride, ry, meta, spairs, cs, gd, acc_ref):
    def step(cell, carry):
        for g in range(STATIC):
            i = cell * stride + g
            base, sp = meta[i], cs[i]
            acc = [acc_ref[i, c] for c in range(3)]
            for slot in layers:
                for b in (0, 1):
                    f = sp + spairs[slot, base + b * (ry + 1), 0]
                    for c in range(3):
                        acc[c] = acc[c] + f * gd[cell * STATIC + g, slot, b, c]
            for c in range(3):
                acc_ref[i, c] = acc[c]
        return carry

    lax.fori_loop(0, cells, step, 0)


def step_kernel(
    sizes, rx, nt, half, count_hbm, pos_hbm, slot_ref, packed, cen, pairs, vs, cs, root_ref,
    spairs, acc_ref, count_ref, pos_ref, own, ext, raw, cent_row, meta, rho, sown, sext, gd,
    load, send, recv, send2, recv2,
):
    loads = [
        pltpu.make_async_copy(count_hbm, count_ref, load.at[0]),
        pltpu.make_async_copy(pos_hbm, pos_ref, load.at[1]),
    ]
    for copy in loads:
        copy.start()
    barrier, arrivals = enter(sizes)
    ry, tiles, cells = 2 * nt, rx * nt, 2 * rx * nt
    width = 2 * half
    kept, slots = layer_slots(sizes[0])
    home = slots[DEPTH]
    groups = group_count(half)
    stride = group_stride(half)
    order = arrival_order(sizes[0])
    for copy in loads:
        copy.wait()
    load_rows(rx, nt, half, home, count_ref, pos_ref, own, ext, raw)
    assign_slots(tiles, half, raw, slot_ref, cent_row, packed)
    spread_centres(tiles, nt, ry, half, groups, stride, slot_ref, cent_row, packed, cen, meta)
    pl.semaphore_wait(barrier, arrivals)
    sends = start_copies(sizes, rx, nt, own, ext, send, recv)

    def arrive(e, own_ref, ext_ref, send_sem, recv_sem, channels, pairs_ref):
        slot, known, _ = order[e]
        wait_layer(sizes, rx, nt, own_ref, ext_ref, send_sem, recv_sem, slot, known)
        build_pairs(slot, 0, rx + 2, ry, half, channels, ext_ref, pairs_ref)

    def density(sides, first, e):
        slot, known, offsets = order[e]
        shifted = []
        for a, z in offsets:
            if known is None:
                shifted.append((a.astype(jnp.float32) * SLIDES[2], z))
            else:
                shifted.append((a * SLIDES[2] if a else None, z))
        density_layer(
            sides, first, slot, shifted, rx, groups, stride, ry, meta, pairs, cen, vs, rho
        )

    both = [(0, 1)] * rx
    inner = [tuple(b for b in (0, 1) if 1 <= x + b and x + b < rx) for x in range(rx)]
    outer = [tuple(b for b in (0, 1) if b not in inner[x]) for x in range(rx)]
    wait_layer(sizes, rx, nt, own, ext, send, recv, home, 0, (0,))
    build_pairs(home, 1, rx + 1, ry, half, 3, ext, pairs)
    density(inner, True, 0)
    wait_layer(sizes, rx, nt, own, ext, send, recv, home, 0, (-1, 1))
    build_pairs(home, 0, 1, ry, half, 3, ext, pairs)
    build_pairs(home, rx + 1, rx + 2, ry, half, 3, ext, pairs)
    density(outer, False, 0)
    for e in range(1, len(order)):
        arrive(e, own, ext, send, recv, 3, pairs)
        density(both, False, e)
    slope_pass(tiles, nt, half, groups, stride, slot_ref, rho, cs, root_ref, sown, sext, home)
    sends += start_copies(sizes, rx, nt, sown, sext, send2, recv2)
    pair_pass(sizes[0], cells, stride, ry, width, meta, pairs, cen, vs, gd, acc_ref)
    for chunk in [(0, 1)] + [(e,) for e in range(2, len(order))]:
        chunk = [e for e in chunk if e < len(order)]
        for e in chunk:
            arrive(e, sown, sext, send2, recv2, 1, spairs)
        layers = [order[e][0] for e in chunk]
        slope_force(layers, cells, stride, ry, meta, spairs, cs, gd, acc_ref)
    for copy in sends:
        copy.wait_send()


def finish_kernel(
    nz, rx, nt, half, slot_ref, packed, cen, pairs, vs, cs, root_ref, spairs, acc_ref,
    force_ref, energy_ref, codes, values,
):
    width, ry, tiles = 2 * half, 2 * nt, rx * nt
    stride = group_stride(half)
    sub = iota((SUB, width), 0).astype(jnp.float32)
    for r in range(tiles):
        for k in (0, 1):
            codes[2 * r + k] = group_code(packed, r, k, half)

    def gather(r, carry):
        slot = slot_ref[r]
        total = [jnp.zeros((SUB, width), jnp.float32) for _ in range(4)]
        for k in (0, 1):
            for g in range(STATIC):
                pick = slot == sub + float(k * width + g * SUB)
                for c in range(4):
                    part = jnp.sum(acc_ref[(2 * r + k) * stride + g, c], axis=1, keepdims=True)
                    total[c] = total[c] + jnp.where(pick, part, 0.0)
        for c in range(4):
            values[r, c] = total[c]
        return carry

    lax.fori_loop(0, tiles, gather, 0, unroll=2)

    def rest(cell, carry):
        r, k = cell // 2, cell % 2
        x, j = r // nt, 2 * (r % nt) + k
        code = codes[cell]

        def group(g, carry):
            i = cell * stride + g
            sp = cs[i]
            xhi, yhi = group_place(code, g)
            base = (x + xhi) * (ry + 1) + j + yhi
            acc = [0.0] * 4
            for slot, b, dens, pair in pair_sums(nz, ry, i, base, pairs, cen, vs):
                f = sp + spairs[slot, base + b * (ry + 1), 0]
                for c in range(3):
                    acc[c] = acc[c] + f * dens[c] + pair[c]
                acc[3] = acc[3] + pair[3]
            pick = slot_ref[r] == sub + (k * width + g * SUB).astype(jnp.float32)
            for c in range(4):
                part = jnp.sum(acc[c], axis=1, keepdims=True)
                values[r, c] = values[r, c] + jnp.where(pick, part, 0.0)
            return carry

        lax.fori_loop(STATIC, code >> 12, group, 0)
        return carry

    lax.fori_loop(0, 2 * tiles, rest, 0)

    for x in range(rx):
        for t in range(nt):
            r = x * nt + t
            for c in range(4):
                value = jnp.sum(values[r, c], axis=0, keepdims=True)
                if c < 3:
                    value = value * (4.0 / 3.0 * G2 / SCALE)
                else:
                    value = value * G2 - 1.0 - root_ref[r]
                value = jnp.where(slot_ref[r] >= 0.0, value, 0.0)
                for k in (0, 1):
                    part = value[:, k * half : (k + 1) * half]
                    if c < 3:
                        force_ref[c, 0, x, 2 * t + k : 2 * t + k + 1, :] = part
                    else:
                        energy_ref[0, x, 2 * t + k : 2 * t + k + 1, :] = part


def group_stride(half):
    return group_count(half)


def body(positions, counts):
    rx, ry, half = positions.shape[2:]
    nt, width = ry // 2, 2 * half
    f32 = jnp.float32
    sizes = tuple(lax.axis_size(axis) for axis in AXES)
    kept, _ = layer_slots(sizes[0])
    layers, tiles, cells = len(kept), rx * nt, rx * ry
    total = cells * group_stride(half)
    rows = (rx + 2) * (ry + 1)

    def vmem(*dims):
        return pltpu.VMEM(dims, f32)

    passed = (
            vmem(tiles, 1, width),
            vmem(tiles, 1, width),
            vmem(total, 3, SUB, width),
            vmem(layers, rows, 3, 1, width),
            vmem(total, LAYERS, 2, SUB, width),
            vmem(total, SUB, width),
            vmem(tiles, 1, width),
            vmem(layers, rows, 1, 1, width),
            vmem(total, 4, SUB, width),
    )
    held = sum(4 * math.prod(ref.shape) for ref in passed)
    shared = pl.pallas_call(
        functools.partial(step_kernel, sizes, rx, nt, half),
        out_shape=passed,
        in_specs=[HBM, HBM],
        out_specs=(VMEM,) * 9,
        scratch_shapes=[
            pltpu.SMEM(counts.shape, jnp.int32),
            vmem(*positions.shape),
            vmem(rx, nt, 3, 1, width),
            vmem(layers, rx + 2, nt + 2, 3, 1, width),
            vmem(3, tiles, width),
            vmem(tiles, 3, 1, width),
            pltpu.SMEM((total,), jnp.int32),
            vmem(total, SUB, width),
            vmem(rx, nt, 1, 1, width),
            vmem(layers, rx + 2, nt + 2, 1, 1, width),
            vmem(cells * STATIC, layers, 2, 3, SUB, width),
            pltpu.SemaphoreType.DMA((2,)),
        ]
        + [pltpu.SemaphoreType.DMA((layers, 9))] * 4,
        compiler_params=pltpu.CompilerParams(
            collective_id=0, has_side_effects=True, vmem_limit_bytes=VMEM_BYTES - held - SPARE
        ),
        name="step",
    )(counts, positions)
    return pl.pallas_call(
        functools.partial(finish_kernel, sizes[0], rx, nt, half),
        out_shape=(
            jax.ShapeDtypeStruct((3, 1, rx, ry, half), f32),
            jax.ShapeDtypeStruct((1, rx, ry, half), f32),
        ),
        in_specs=[VMEM] * 9,
        out_specs=(VMEM, VMEM),
        scratch_shapes=[pltpu.SMEM((cells,), jnp.int32), vmem(tiles, 4, SUB, width)],
        compiler_params=pltpu.CompilerParams(vmem_limit_bytes=24 * 2**20),
        name="finish",
    )(*shared)


def solution(mesh):
    return jax.shard_map(
        body,
        mesh=mesh,
        in_specs=(P(None, "gz", "gx", "gy", None), P("gz", "gx", "gy")),
        out_specs=(P(None, "gz", "gx", "gy", None), P("gz", "gx", "gy", None)),
        check_vma=False,
    )
```

```python
import functools
import math

import jax
import jax.numpy as jnp
from jax import lax
from jax.experimental import pallas as pl
from jax.experimental.pallas import tpu as pltpu
from jax.sharding import PartitionSpec as P

CUT = 4.95
SIDES = (12.0, 12.0, 2.5)
FAR = 1024.0
LOG2E = math.log2(math.e)
SCALE = math.sqrt(LOG2E / 8.0)
REACH = CUT * CUT * LOG2E / 8.0
SPLIT = 0.5
SLIDES = tuple(side * SCALE for side in SIDES)
A = 2.0 * LOG2E
B = 0.75 * LOG2E
G1 = 2.0 ** (-REACH) / REACH**2
G2 = 2.0 ** (-REACH * 8.0 / 3.0) / REACH**2
SIGMA = (3.0 / 16.0) * G1 / G2
CLASSES = 4
SUB = 8
STATIC = 8
VMEM_BYTES = 67_043_328
SPARE = 16384
DEPTH = 2
LAYERS = 2 * DEPTH + 1
VMEM = pl.BlockSpec(memory_space=pltpu.VMEM)
HBM = pl.BlockSpec(memory_space=pltpu.HBM)


AXES = ("gz", "gx", "gy")


def layer_slots(nz):
    kept = []
    for a in range(-DEPTH, DEPTH + 1):
        if all((a - k) % nz for k in kept):
            kept.append(a)
    slot = [
        next(i for i, k in enumerate(kept) if (a - k) % nz == 0)
        for a in range(-DEPTH, DEPTH + 1)
    ]
    return kept, slot


def displacements(sizes):
    kept, _ = layer_slots(sizes[0])
    copies, others = [], []
    for s, a in enumerate(kept):
        for b in (-1, 0, 1):
            for c in (-1, 0, 1):
                if (a, b, c) == (0, 0, 0):
                    continue
                step = tuple(-o % n for o, n in zip((a, b, c), sizes))
                copies.append((s, b, c, step))
                if any(step) and step not in others:
                    others.append(step)
    return copies, others


def device(step, sizes):
    return {
        axis: lax.rem(lax.axis_index(axis) + d + n, n)
        for axis, d, n in zip(AXES, step, sizes)
    }


def enter(sizes):
    _, others = displacements(sizes)
    barrier = pltpu.get_barrier_semaphore()
    for step in others:
        pl.semaphore_signal(
            barrier,
            inc=1,
            device_id=device(step, sizes),
            device_id_type=pl.DeviceIdType.MESH,
        )
    return barrier, len(others)


def edge(offset, length):
    if offset == 0:
        return pl.ds(0, length), pl.ds(1, length)
    if offset < 0:
        return pl.ds(length - 1, 1), pl.ds(0, 1)
    return pl.ds(0, 1), pl.ds(length + 1, 1)


def link(sizes, rx, nt, own, ext, send, recv, slot, b, c, step):
    (sx, dx), (st, dt) = edge(b, rx), edge(c, nt)
    source, target = own.at[sx, st], ext.at[slot, dx, dt]
    j = 3 * (b + 1) + c + 1
    if step is None:
        return pltpu.make_async_copy(source, target, recv.at[slot, j])
    return pltpu.make_async_remote_copy(
        src_ref=source,
        dst_ref=target,
        send_sem=send.at[slot, j],
        recv_sem=recv.at[slot, j],
        device_id=device(step, sizes),
        device_id_type=pl.DeviceIdType.MESH,
    )


def layer_links(sizes, rx, nt, own, ext, send, recv, slot, dz, sides=(-1, 0, 1)):
    found = []
    for b in sides:
        for c in (-1, 0, 1):
            step = (dz, -b, -c)
            if isinstance(dz, int):
                step = tuple(d % n for d, n in zip(step, sizes))
                if (dz, b, c) == (0, 0, 0):
                    continue
                if not any(step):
                    step = None
            copy = link(sizes, rx, nt, own, ext, send, recv, slot, b, c, step)
            found.append((copy, step is not None))
    return found


def start_layer(*where):
    for copy, _ in layer_links(*where):
        copy.start()


def wait_layer(*where):
    for copy, remote in layer_links(*where):
        if remote:
            copy.wait_recv()
        else:
            copy.wait()


def start_copies(sizes, rx, nt, own, ext, send, recv):
    nz = sizes[0]
    place = (sizes, rx, nt, own, ext, send, recv)
    kept, slots = layer_slots(nz)
    start_layer(*place, slots[DEPTH], 0)
    if nz < 4:
        for slot, a in enumerate(kept):
            if a:
                start_layer(*place, slot, -a)
        return
    near, middle = nearest(nz)

    def start_far():
        start_layer(*place, DEPTH + near, -near)

    start_layer(*place, DEPTH - near, near)
    pl.when(middle)(start_far)
    for slot in sorted({slots[0], slots[2 * DEPTH]}):
        start_layer(*place, slot, -kept[slot])
    pl.when(jnp.logical_not(middle))(start_far)


def wait_sends(sizes, rx, nt, own, ext, send, recv):
    for slot, a in enumerate(layer_slots(sizes[0])[0]):
        for copy, remote in layer_links(sizes, rx, nt, own, ext, send, recv, slot, -a):
            if remote:
                copy.wait_send()


def nearest(nz):
    z = lax.axis_index("gz")
    return jnp.where(lax.rem(z, 2) == 0, 1, -1), (z != 0) & (z != nz - 1)


def offsets_of(nz, slot):
    return [a for a in range(-DEPTH, DEPTH + 1) if layer_slots(nz)[1][a + DEPTH] == slot]


def arrival_order(nz):
    kept, slots = layer_slots(nz)
    home = slots[DEPTH]
    if nz < 4:
        rest = [s for s in range(len(kept)) if s != home]
        return [(s, kept[s], [(a, a + DEPTH) for a in offsets_of(nz, s)]) for s in [home] + rest]
    near, _ = nearest(nz)
    order = [(home, 0, [(0, DEPTH)]), (near + DEPTH, None, [(near, near + DEPTH)])]
    for s in sorted({slots[0], slots[2 * DEPTH]}):
        order.append((s, kept[s], [(a, a + DEPTH) for a in offsets_of(nz, s)]))
    order.append((DEPTH - near, None, [(-near, DEPTH - near)]))
    return order


def iota(shape, dim):
    return lax.broadcasted_iota(jnp.int32, shape, dim)


def group_count(half):
    return (half + CLASSES * (SUB - 1)) // SUB


def load_rows(rx, nt, half, home, count_ref, pos_ref, own, ext, raw):
    lane = iota((1, 2 * half), 1)
    for x in range(rx):
        for t in range(nt):
            n0, n1 = count_ref[0, x, 2 * t], count_ref[0, x, 2 * t + 1]
            occupied = jnp.where(lane < half, lane - n0, lane - half - n1) < 0
            for c in range(3):
                rows = [pos_ref[c, 0, x, 2 * t + k : 2 * t + k + 1, :] for k in (0, 1)]
                row = jnp.concatenate(rows, axis=1)
                raw[c, pl.ds(x * nt + t, 1)] = jnp.where(occupied, row, FAR)
                row = jnp.where(occupied, row * SLIDES[c], FAR)
                own[x, t, c] = row
                ext[home, x + 1, t + 1, c] = row


def assign_slots(tiles, half, raw, slot_ref, cent_row, packed):
    width = 2 * half
    u, v, w = raw[0], raw[1], raw[2]
    here = u < 0.5 * FAR
    xhi, yhi = u >= SPLIT, v >= SPLIT
    masks = [
        here & ~xhi & ~yhi,
        here & ~xhi & yhi,
        here & xhi & ~yhi,
        here & xhi & yhi,
    ]
    ones = [jnp.where(m, 1.0, 0.0) for m in masks]
    i, j = iota((width, width), 0), iota((width, width), 1)
    same = i // half == j // half
    before = jnp.where(same & (i < j), 1.0, 0.0)
    whole = jnp.where(same, 1.0, 0.0)
    stacked = jnp.concatenate(ones, axis=0)
    ranks = jnp.dot(stacked, before, preferred_element_type=jnp.float32)
    totals = jnp.dot(stacked, whole, preferred_element_type=jnp.float32)
    upper = iota((tiles, width), 1) >= half
    slot = jnp.where(here, jnp.where(upper, float(width), 0.0), -2.0 * width)
    ends = jnp.zeros((tiles, width), jnp.float32)
    pack = jnp.zeros((tiles, width), jnp.float32)
    for k in range(CLASSES):
        rank, total = ranks[k * tiles : (k + 1) * tiles], totals[k * tiles : (k + 1) * tiles]
        slot = slot + ones[k] * (ends * SUB + rank)
        ends = ends + jnp.floor((total + (SUB - 1)) * (1.0 / SUB))
        pack = pack + ends * float(16**k)
    px = u * SLIDES[0] + jnp.where(xhi, 0.0, SLIDES[0])
    py = v * SLIDES[1] + jnp.where(yhi, 0.0, SLIDES[1])
    pz = w * SLIDES[2]
    for r in range(tiles):
        slot_ref[r] = slot[r : r + 1]
        packed[r] = pack[r : r + 1]
        for c, p in enumerate((px, py, pz)):
            cent_row[r, c] = p[r : r + 1]


def group_code(packed, r, k, half):
    lane = iota((1, 2 * half), 1)
    return jnp.sum(jnp.where(lane == k * half, packed[r], 0.0)).astype(jnp.int32)


def group_place(code, g):
    b1, b2, b3 = code & 15, (code >> 4) & 15, (code >> 8) & 15
    xhi = jnp.where(b2 <= g, 1, 0)
    yhi = jnp.where(b3 <= g, 1, jnp.where(b2 <= g, 0, jnp.where(b1 <= g, 1, 0)))
    return xhi, yhi


def spread_centres(tiles, nt, ry, half, groups, stride, slot_ref, cent_row, packed, cen, dens, meta):
    width = 2 * half
    sub = iota((SUB, width), 0).astype(jnp.float32)
    lean = jnp.where(iota((SUB, width), 1) >= half, 0.5 * SLIDES[1], -0.5 * SLIDES[1])

    def step(r, carry):
        slot = slot_ref[r]
        rows = [cent_row[r, c] for c in range(3)]
        x, t = r // nt, r % nt
        for k in (0, 1):
            code = group_code(packed, r, k, half)
            for g in range(groups):
                i = (2 * r + k) * stride + g
                xhi, yhi = group_place(code, g)
                meta[i] = (x + xhi) * (ry + 1) + 2 * t + k + yhi
                sign = jnp.where(yhi == k, -1.0, 1.0)
                pick = slot == sub + float(k * width + g * SUB)
                p = []
                for c in range(3):
                    column = jnp.sum(jnp.where(pick, rows[c], 0.0), axis=1, keepdims=True)
                    wide = jnp.broadcast_to(column, (SUB, width))
                    if c == 1:
                        wide = wide - (0.5 * SLIDES[1] + sign * lean)
                    cen[i, c] = wide
                    dens[i, c] = wide + wide
                    p.append(wide)
                flat = (REACH - p[1] * p[1]) - p[2] * p[2]
                next_x = p[0] - SLIDES[0]
                dens[i, 3] = flat - p[0] * p[0]
                dens[i, 4] = flat - next_x * next_x
        return carry

    lax.fori_loop(0, tiles, step, 0, unroll=2)


def pair_row(rows, p, half):
    if p % 2:
        return rows[(p + 1) // 2]
    low = iota((1, 2 * half), 1) < half
    return jnp.where(low, rows[p // 2 + 1], rows[p // 2])


def build_pairs(s, first, last, ry, half, shifts, ext, pairs):
    def step(x, carry):
        rows = [[ext[s, x, t, c] for t in range(ry // 2 + 2)] for c in range(3)]
        for p in range(ry + 1):
            at = x * (ry + 1) + p
            qx, qy, qz = (pair_row(rows[c], p, half) for c in range(3))
            pairs[s, at, 0], pairs[s, at, 1] = qx, qy
            flat = qx * qx + qy * qy
            for k, shift in enumerate(shifts):
                q = qz if shift is None else qz + shift
                pairs[s, at, 2 + 2 * k] = q
                pairs[s, at, 3 + 2 * k] = -(flat + q * q)
        return carry

    lax.fori_loop(first, last, step, 0, unroll=2 if (last - first) % 2 == 0 else 1)


def build_slopes(s, cols, ry, half, ext, pairs):
    def step(x, carry):
        rows = [ext[s, x, t, 0] for t in range(ry // 2 + 2)]
        for p in range(ry + 1):
            pairs[s, x * (ry + 1) + p, 0] = pair_row(rows, p, half)
        return carry

    lax.fori_loop(0, cols, step, 0, unroll=2)


def density_layer(
    sides, first, slot, offsets, rx, groups, stride, ry, meta, pairs, table, vs, rho
):
    def run(x_cell):
        def step(j, carry):
            for g in range(groups):
                i = (x_cell * ry + j) * stride + g
                base = meta[i]
                x, y, w = table[i, 0], table[i, 1], table[i, 2]
                total = None if first else rho[i]
                for b in sides[x_cell]:
                    at = base + b * (ry + 1)
                    qx, qy = pairs[slot, at, 0], pairs[slot, at, 1]
                    xb = x - 2.0 * SLIDES[0] if b else x
                    flat = (table[i, 3 + b] + xb * qx) + y * qy
                    for k, z in enumerate(offsets):
                        qz, cq = pairs[slot, at, 2 + 2 * k], pairs[slot, at, 3 + 2 * k]
                        v = jnp.maximum(flat + (cq + w * qz), 0.0)
                        vs[i, z, b] = v
                        part = jnp.exp2(v) * (v * v)
                        total = part if total is None else total + part
                rho[i] = jnp.zeros_like(x) if total is None else total
            return carry

        return step

    for x_cell in range(rx):
        if sides[x_cell] or first:
            lax.fori_loop(0, ry, run(x_cell), 0, unroll=2)


def slope_pass(tiles, nt, half, groups, stride, slot_ref, rho, cs, root_ref, sown, sext, home):
    width = 2 * half
    sub = iota((SUB, width), 0).astype(jnp.float32)

    def step(r, carry):
        slot = slot_ref[r]
        value = jnp.zeros((SUB, width), jnp.float32)
        for k in (0, 1):
            for g in range(groups):
                i = (2 * r + k) * stride + g
                one_rho = jnp.sum(rho[i], axis=1, keepdims=True) * G1
                value = value + jnp.where(
                    slot == sub + float(k * width + g * SUB), one_rho, 0.0
                )
                one_rho = jnp.broadcast_to(one_rho, (SUB, width))
                cs[i] = (-0.5 * SIGMA) * lax.rsqrt(jnp.maximum(one_rho, 0.5))
        one_rho = jnp.sum(value, axis=0, keepdims=True)
        root = jnp.sqrt(jnp.where(slot >= 0.0, one_rho, 1.0))
        root_ref[r] = root
        row = (-0.5 * SIGMA) / root
        x, t = r // nt, r % nt
        sown[x, t, 0] = row
        sext[home, x + 1, t + 1, 0] = row
        return carry

    lax.fori_loop(0, tiles, step, 0, unroll=4)


def pair_terms(v):
    g = jnp.exp2(v) * ((v + A) * v)
    w = v * jnp.exp2(v * (8.0 / 3.0))
    return g, w * (v + B), w * v


def pair_sums(nz, spots, ry, i, base, pairs, cen, vs):
    x, y, w = cen[i, 0], cen[i, 1], cen[i, 2]
    for slot, b in spots:
        at = base + b * (ry + 1)
        dx = (x - SLIDES[0] if b else x) - pairs[slot, at, 0]
        dy = y - pairs[slot, at, 1]
        dens = pair = phi = dens_z = pair_z = 0.0
        for k, a in enumerate(offsets_of(nz, slot)):
            dz = w - pairs[slot, at, 2 + 2 * k]
            d, p, f = pair_terms(vs[i, a + DEPTH, b])
            dens, pair, phi = dens + d, pair + p, phi + f
            dens_z, pair_z = dens_z + d * dz, pair_z + p * dz
        yield slot, b, (dens * dx, dens * dy, dens_z), (pair * dx, pair * dy, pair_z, phi)


def pair_pass(
    nz, spots, first, rx, stride, ry, width, meta, pairs, cen, vs, gd, acc_ref
):
    def run(x_cell):
        def step(j, carry):
            cell = x_cell * ry + j
            for g in range(STATIC):
                i = cell * stride + g
                if first:
                    acc = [jnp.zeros((SUB, width), jnp.float32)] * 4
                else:
                    acc = [acc_ref[i, c] for c in range(4)]
                sums = pair_sums(nz, spots[x_cell], ry, i, meta[i], pairs, cen, vs)
                for slot, b, dens, pair in sums:
                    for c in range(3):
                        gd[cell * STATIC + g, slot, b, c] = dens[c]
                    acc = [total + part for total, part in zip(acc, pair)]
                for c in range(4):
                    acc_ref[i, c] = acc[c]
            return carry

        return step

    for x_cell in range(rx):
        if spots[x_cell] or first:
            lax.fori_loop(0, ry, run(x_cell), 0)


def slope_force(layers, cells, stride, ry, meta, spairs, cs, gd, acc_ref):
    def step(cell, carry):
        for g in range(STATIC):
            i = cell * stride + g
            base, sp = meta[i], cs[i]
            acc = [acc_ref[i, c] for c in range(3)]
            for slot in layers:
                for b in (0, 1):
                    f = sp + spairs[slot, base + b * (ry + 1), 0]
                    for c in range(3):
                        acc[c] = acc[c] + f * gd[cell * STATIC + g, slot, b, c]
            for c in range(3):
                acc_ref[i, c] = acc[c]
        return carry

    lax.fori_loop(0, cells, step, 0)


def step_kernel(
    sizes, rx, nt, half, count_hbm, pos_hbm, slot_ref, packed, cen, pairs, vs, cs, root_ref,
    spairs, acc_ref, count_ref, pos_ref, own, ext, raw, cent_row, meta, rho, sown, sext, gd, table, load, send, recv, send2, recv2,
):
    loads = [
        pltpu.make_async_copy(count_hbm, count_ref, load.at[0]),
        pltpu.make_async_copy(pos_hbm, pos_ref, load.at[1]),
    ]
    for copy in loads:
        copy.start()
    barrier, arrivals = enter(sizes)
    ry, tiles, cells = 2 * nt, rx * nt, 2 * rx * nt
    width = 2 * half
    kept, slots = layer_slots(sizes[0])
    home = slots[DEPTH]
    groups = group_count(half)
    stride = group_stride(half)
    order = arrival_order(sizes[0])
    for copy in loads:
        copy.wait()
    load_rows(rx, nt, half, home, count_ref, pos_ref, own, ext, raw)
    assign_slots(tiles, half, raw, slot_ref, cent_row, packed)
    spread_centres(tiles, nt, ry, half, groups, stride, slot_ref, cent_row, packed, cen, table, meta)
    pl.semaphore_wait(barrier, arrivals)
    where = (sizes, rx, nt, own, ext, send, recv)
    swhere = (sizes, rx, nt, sown, sext, send2, recv2)
    start_copies(*where)

    def arrive(e, place):
        slot, known, _ = order[e]
        wait_layer(*place, slot, 1 if known is None else -known)

    def shifts_of(e):
        _, known, offsets = order[e]
        if known is None:
            return [offsets[0][0].astype(jnp.float32) * SLIDES[2]]
        return [a * SLIDES[2] if a else None for a, _ in offsets]

    def density(sides, first, e):
        slot, _, offsets = order[e]
        zs = [z for _, z in offsets]
        density_layer(
            sides, first, slot, zs, rx, groups, stride, ry, meta, pairs, table, vs, rho
        )

    def pairwise(spots, first):
        pair_pass(
            sizes[0], spots, first, rx, stride, ry, width, meta, pairs, cen, vs, gd, acc_ref
        )

    def pair_home(sides, first):
        pairwise([[(home, b) for b in side] for side in sides], first)

    both = [(0, 1)] * rx
    inner = [tuple(b for b in (0, 1) if 1 <= x + b and x + b < rx) for x in range(rx)]
    outer = [tuple(b for b in (0, 1) if b not in inner[x]) for x in range(rx)]
    wait_layer(*where, home, 0, (0,))
    build_pairs(home, 1, rx + 1, ry, half, [None], ext, pairs)
    density(inner, True, 0)
    wait_layer(*where, home, 0, (-1, 1))
    build_pairs(home, 0, 1, ry, half, [None], ext, pairs)
    build_pairs(home, rx + 1, rx + 2, ry, half, [None], ext, pairs)
    density(outer, False, 0)
    pair_home(inner, True)

    def take(e):
        arrive(e, where)
        build_pairs(order[e][0], 0, rx + 2, ry, half, shifts_of(e), ext, pairs)
        density(both, False, e)

    last = len(order) - 1
    if sizes[0] < 4:
        for e in range(1, len(order)):
            take(e)
        pair_home(outer, False)
    else:
        _, middle = nearest(sizes[0])
        take(1)
        pl.when(middle)(lambda: take(last))
        for e in range(2, last):
            take(e)
        pl.when(jnp.logical_not(middle))(lambda: take(last))
    slope_pass(tiles, nt, half, groups, stride, slot_ref, rho, cs, root_ref, sown, sext, home)
    start_copies(*swhere)
    pair_home(outer, False)
    away = [(s, b) for s in range(len(kept)) if s != home for b in (0, 1)]
    pairwise([away] * rx, False)
    for chunk in [(0, 1)] + [(e,) for e in range(2, len(order))]:
        chunk = [e for e in chunk if e < len(order)]
        for e in chunk:
            arrive(e, swhere)
            build_slopes(order[e][0], rx + 2, ry, half, sext, spairs)
        layers = [order[e][0] for e in chunk]
        slope_force(layers, cells, stride, ry, meta, spairs, cs, gd, acc_ref)
    wait_sends(*where)
    wait_sends(*swhere)


def finish_kernel(
    nz, rx, nt, half, slot_ref, packed, cen, pairs, vs, cs, root_ref, spairs, acc_ref,
    force_ref, energy_ref, codes, values,
):
    width, ry, tiles = 2 * half, 2 * nt, rx * nt
    stride = group_stride(half)
    sub = iota((SUB, width), 0).astype(jnp.float32)
    spots = [(s, b) for s in range(len(layer_slots(nz)[0])) for b in (0, 1)]
    for r in range(tiles):
        for k in (0, 1):
            codes[2 * r + k] = group_code(packed, r, k, half)

    def gather(r, carry):
        slot = slot_ref[r]
        total = [jnp.zeros((SUB, width), jnp.float32) for _ in range(4)]
        for k in (0, 1):
            for g in range(STATIC):
                pick = slot == sub + float(k * width + g * SUB)
                for c in range(4):
                    part = jnp.sum(acc_ref[(2 * r + k) * stride + g, c], axis=1, keepdims=True)
                    total[c] = total[c] + jnp.where(pick, part, 0.0)
        for c in range(4):
            values[r, c] = total[c]
        return carry

    lax.fori_loop(0, tiles, gather, 0, unroll=4)

    def rest(cell, carry):
        r, k = cell // 2, cell % 2
        x, j = r // nt, 2 * (r % nt) + k
        code = codes[cell]

        def group(g, carry):
            i = cell * stride + g
            sp = cs[i]
            xhi, yhi = group_place(code, g)
            base = (x + xhi) * (ry + 1) + j + yhi
            acc = [0.0] * 4
            for slot, b, dens, pair in pair_sums(nz, spots, ry, i, base, pairs, cen, vs):
                f = sp + spairs[slot, base + b * (ry + 1), 0]
                for c in range(3):
                    acc[c] = acc[c] + f * dens[c] + pair[c]
                acc[3] = acc[3] + pair[3]
            pick = slot_ref[r] == sub + (k * width + g * SUB).astype(jnp.float32)
            for c in range(4):
                part = jnp.sum(acc[c], axis=1, keepdims=True)
                values[r, c] = values[r, c] + jnp.where(pick, part, 0.0)
            return carry

        lax.fori_loop(STATIC, code >> 12, group, 0)
        return carry

    lax.fori_loop(0, 2 * tiles, rest, 0)

    for x in range(rx):
        for t in range(nt):
            r = x * nt + t
            for c in range(4):
                value = jnp.sum(values[r, c], axis=0, keepdims=True)
                if c < 3:
                    value = value * (4.0 / 3.0 * G2 / SCALE)
                else:
                    value = value * G2 - 1.0 - root_ref[r]
                value = jnp.where(slot_ref[r] >= 0.0, value, 0.0)
                for k in (0, 1):
                    part = value[:, k * half : (k + 1) * half]
                    if c < 3:
                        force_ref[c, 0, x, 2 * t + k : 2 * t + k + 1, :] = part
                    else:
                        energy_ref[0, x, 2 * t + k : 2 * t + k + 1, :] = part


def group_stride(half):
    return group_count(half)


def body(positions, counts):
    rx, ry, half = positions.shape[2:]
    nt, width = ry // 2, 2 * half
    f32 = jnp.float32
    sizes = tuple(lax.axis_size(axis) for axis in AXES)
    kept, _ = layer_slots(sizes[0])
    layers, tiles, cells = len(kept), rx * nt, rx * ry
    total = cells * group_stride(half)
    rows = (rx + 2) * (ry + 1)
    channels = 2 + 2 * max(len(offsets_of(sizes[0], s)) for s in range(layers))

    def vmem(*dims):
        return pltpu.VMEM(dims, f32)

    passed = (
            vmem(tiles, 1, width),
            vmem(tiles, 1, width),
            vmem(total, 3, SUB, width),
            vmem(layers, rows, channels, 1, width),
            vmem(total, LAYERS, 2, SUB, width),
            vmem(total, SUB, width),
            vmem(tiles, 1, width),
            vmem(layers, rows, 1, 1, width),
            vmem(total, 4, SUB, width),
    )
    held = sum(4 * math.prod(ref.shape) for ref in passed)
    shared = pl.pallas_call(
        functools.partial(step_kernel, sizes, rx, nt, half),
        out_shape=passed,
        in_specs=[HBM, HBM],
        out_specs=(VMEM,) * len(passed),
        scratch_shapes=[
            pltpu.SMEM(counts.shape, jnp.int32),
            vmem(*positions.shape),
            vmem(rx, nt, 3, 1, width),
            vmem(layers, rx + 2, nt + 2, 3, 1, width),
            vmem(3, tiles, width),
            vmem(tiles, 3, 1, width),
            pltpu.SMEM((total,), jnp.int32),
            vmem(total, SUB, width),
            vmem(rx, nt, 1, 1, width),
            vmem(layers, rx + 2, nt + 2, 1, 1, width),
            vmem(cells * STATIC, layers, 2, 3, SUB, width),
            vmem(total, 5, SUB, width),
            pltpu.SemaphoreType.DMA((2,)),
        ]
        + [pltpu.SemaphoreType.DMA((layers, 9))] * 4,
        compiler_params=pltpu.CompilerParams(
            collective_id=0, has_side_effects=True, vmem_limit_bytes=VMEM_BYTES - held - SPARE
        ),
        name="step",
    )(counts, positions)
    return pl.pallas_call(
        functools.partial(finish_kernel, sizes[0], rx, nt, half),
        out_shape=(
            jax.ShapeDtypeStruct((3, 1, rx, ry, half), f32),
            jax.ShapeDtypeStruct((1, rx, ry, half), f32),
        ),
        in_specs=[VMEM] * len(passed),
        out_specs=(VMEM, VMEM),
        scratch_shapes=[pltpu.SMEM((cells,), jnp.int32), vmem(tiles, 4, SUB, width)],
        compiler_params=pltpu.CompilerParams(vmem_limit_bytes=24 * 2**20),
        name="finish",
    )(*shared)


def solution(mesh):
    return jax.shard_map(
        body,
        mesh=mesh,
        in_specs=(P(None, "gz", "gx", "gy", None), P("gz", "gx", "gy")),
        out_specs=(P(None, "gz", "gx", "gy", None), P("gz", "gx", "gy", None)),
        check_vma=False,
    )
```

```python
import functools
import math

import jax
import jax.numpy as jnp
from jax import lax
from jax.experimental import pallas as pl
from jax.experimental.pallas import tpu as pltpu
from jax.sharding import PartitionSpec as P

CUT = 4.95
SIDES = (12.0, 12.0, 2.5)
FAR = 1024.0
LOG2E = math.log2(math.e)
SCALE = math.sqrt(LOG2E / 8.0)
REACH = CUT * CUT * LOG2E / 8.0
SPLIT = 0.5
SLIDES = tuple(side * SCALE for side in SIDES)
A = 2.0 * LOG2E
B = 0.75 * LOG2E
G1 = 2.0 ** (-REACH) / REACH**2
G2 = 2.0 ** (-REACH * 8.0 / 3.0) / REACH**2
SIGMA = (3.0 / 16.0) * G1 / G2
CLASSES = 4
SUB = 8
STATIC = 8
VMEM_BYTES = 67_043_328
SPARE = 16384
DEPTH = 2
LAYERS = 2 * DEPTH + 1
VMEM = pl.BlockSpec(memory_space=pltpu.VMEM)
HBM = pl.BlockSpec(memory_space=pltpu.HBM)


AXES = ("gz", "gx", "gy")


def layer_slots(nz):
    kept = []
    for a in range(-DEPTH, DEPTH + 1):
        if all((a - k) % nz for k in kept):
            kept.append(a)
    slot = [
        next(i for i, k in enumerate(kept) if (a - k) % nz == 0)
        for a in range(-DEPTH, DEPTH + 1)
    ]
    return kept, slot


def displacements(sizes):
    kept, _ = layer_slots(sizes[0])
    copies, others = [], []
    for s, a in enumerate(kept):
        for b in (-1, 0, 1):
            for c in (-1, 0, 1):
                if (a, b, c) == (0, 0, 0):
                    continue
                step = tuple(-o % n for o, n in zip((a, b, c), sizes))
                copies.append((s, b, c, step))
                if any(step) and step not in others:
                    others.append(step)
    return copies, others


def device(step, sizes):
    return {
        axis: lax.rem(lax.axis_index(axis) + d + n, n)
        for axis, d, n in zip(AXES, step, sizes)
    }


def enter(sizes):
    _, others = displacements(sizes)
    barrier = pltpu.get_barrier_semaphore()
    for step in others:
        pl.semaphore_signal(
            barrier,
            inc=1,
            device_id=device(step, sizes),
            device_id_type=pl.DeviceIdType.MESH,
        )
    return barrier, len(others)


def edge(offset, length):
    if offset == 0:
        return pl.ds(0, length), pl.ds(1, length)
    if offset < 0:
        return pl.ds(length - 1, 1), pl.ds(0, 1)
    return pl.ds(0, 1), pl.ds(length + 1, 1)


def link(sizes, rx, nt, own, ext, send, recv, slot, b, c, step):
    (sx, dx), (st, dt) = edge(b, rx), edge(c, nt)
    source, target = own.at[sx, st], ext.at[slot, dx, dt]
    j = 3 * (b + 1) + c + 1
    if step is None:
        return pltpu.make_async_copy(source, target, recv.at[slot, j])
    return pltpu.make_async_remote_copy(
        src_ref=source,
        dst_ref=target,
        send_sem=send.at[slot, j],
        recv_sem=recv.at[slot, j],
        device_id=device(step, sizes),
        device_id_type=pl.DeviceIdType.MESH,
    )


def layer_links(sizes, rx, nt, own, ext, send, recv, slot, dz, sides=(-1, 0, 1)):
    found = []
    for b in sides:
        for c in (-1, 0, 1):
            step = (dz, -b, -c)
            if isinstance(dz, int):
                step = tuple(d % n for d, n in zip(step, sizes))
                if (dz, b, c) == (0, 0, 0):
                    continue
                if not any(step):
                    step = None
            copy = link(sizes, rx, nt, own, ext, send, recv, slot, b, c, step)
            found.append((copy, step is not None))
    return found


def start_layer(*where):
    for copy, _ in layer_links(*where):
        copy.start()


def wait_layer(*where):
    for copy, remote in layer_links(*where):
        if remote:
            copy.wait_recv()
        else:
            copy.wait()


def start_copies(sizes, rx, nt, own, ext, send, recv):
    nz = sizes[0]
    place = (sizes, rx, nt, own, ext, send, recv)
    kept, slots = layer_slots(nz)
    start_layer(*place, slots[DEPTH], 0)
    if nz < 4:
        for slot, a in enumerate(kept):
            if a:
                start_layer(*place, slot, -a)
        return
    near, middle = nearest(nz)

    def start_far():
        start_layer(*place, DEPTH + near, -near)

    start_layer(*place, DEPTH - near, near)
    pl.when(middle)(start_far)
    for slot in sorted({slots[0], slots[2 * DEPTH]}):
        start_layer(*place, slot, -kept[slot])
    pl.when(jnp.logical_not(middle))(start_far)


def wait_sends(sizes, rx, nt, own, ext, send, recv):
    for slot, a in enumerate(layer_slots(sizes[0])[0]):
        for copy, remote in layer_links(sizes, rx, nt, own, ext, send, recv, slot, -a):
            if remote:
                copy.wait_send()


def nearest(nz):
    z = lax.axis_index("gz")
    return jnp.where(lax.rem(z, 2) == 0, 1, -1), (z != 0) & (z != nz - 1)


def offsets_of(nz, slot):
    return [a for a in range(-DEPTH, DEPTH + 1) if layer_slots(nz)[1][a + DEPTH] == slot]


def arrival_order(nz):
    kept, slots = layer_slots(nz)
    home = slots[DEPTH]
    if nz < 4:
        rest = [s for s in range(len(kept)) if s != home]
        return [(s, kept[s], [(a, a + DEPTH) for a in offsets_of(nz, s)]) for s in [home] + rest]
    near, _ = nearest(nz)
    order = [(home, 0, [(0, DEPTH)]), (near + DEPTH, None, [(near, near + DEPTH)])]
    for s in sorted({slots[0], slots[2 * DEPTH]}):
        order.append((s, kept[s], [(a, a + DEPTH) for a in offsets_of(nz, s)]))
    order.append((DEPTH - near, None, [(-near, DEPTH - near)]))
    return order


def iota(shape, dim):
    return lax.broadcasted_iota(jnp.int32, shape, dim)


def group_count(half):
    return (half + CLASSES * (SUB - 1)) // SUB


def load_rows(rx, nt, half, home, count_ref, pos_ref, own, ext, raw):
    lane = iota((1, 2 * half), 1)
    for x in range(rx):
        for t in range(nt):
            n0, n1 = count_ref[0, x, 2 * t], count_ref[0, x, 2 * t + 1]
            occupied = jnp.where(lane < half, lane - n0, lane - half - n1) < 0
            for c in range(3):
                rows = [pos_ref[c, 0, x, 2 * t + k : 2 * t + k + 1, :] for k in (0, 1)]
                row = jnp.concatenate(rows, axis=1)
                raw[c, pl.ds(x * nt + t, 1)] = jnp.where(occupied, row, FAR)
                row = jnp.where(occupied, row * SLIDES[c], FAR)
                own[x, t, c] = row
                ext[home, x + 1, t + 1, c] = row


def assign_slots(tiles, half, raw, slot_ref, cent_row, packed):
    width = 2 * half
    u, v, w = raw[0], raw[1], raw[2]
    here = u < 0.5 * FAR
    xhi, yhi = u >= SPLIT, v >= SPLIT
    masks = [
        here & ~xhi & ~yhi,
        here & ~xhi & yhi,
        here & xhi & ~yhi,
        here & xhi & yhi,
    ]
    ones = [jnp.where(m, 1.0, 0.0) for m in masks]
    i, j = iota((width, width), 0), iota((width, width), 1)
    same = i // half == j // half
    before = jnp.where(same & (i < j), 1.0, 0.0)
    whole = jnp.where(same, 1.0, 0.0)
    stacked = jnp.concatenate(ones, axis=0)
    ranks = jnp.dot(stacked, before, preferred_element_type=jnp.float32)
    totals = jnp.dot(stacked, whole, preferred_element_type=jnp.float32)
    upper = iota((tiles, width), 1) >= half
    slot = jnp.where(here, jnp.where(upper, float(width), 0.0), -2.0 * width)
    ends = jnp.zeros((tiles, width), jnp.float32)
    pack = jnp.zeros((tiles, width), jnp.float32)
    for k in range(CLASSES):
        rank, total = ranks[k * tiles : (k + 1) * tiles], totals[k * tiles : (k + 1) * tiles]
        slot = slot + ones[k] * (ends * SUB + rank)
        ends = ends + jnp.floor((total + (SUB - 1)) * (1.0 / SUB))
        pack = pack + ends * float(16**k)
    px = u * SLIDES[0] + jnp.where(xhi, 0.0, SLIDES[0])
    py = v * SLIDES[1] + jnp.where(yhi, 0.0, SLIDES[1])
    pz = w * SLIDES[2]
    for r in range(tiles):
        slot_ref[r] = slot[r : r + 1]
        packed[r] = pack[r : r + 1]
        for c, p in enumerate((px, py, pz)):
            cent_row[r, c] = p[r : r + 1]


def group_code(packed, r, k, half):
    lane = iota((1, 2 * half), 1)
    return jnp.sum(jnp.where(lane == k * half, packed[r], 0.0)).astype(jnp.int32)


def group_place(code, g):
    b1, b2, b3 = code & 15, (code >> 4) & 15, (code >> 8) & 15
    xhi = jnp.where(b2 <= g, 1, 0)
    yhi = jnp.where(b3 <= g, 1, jnp.where(b2 <= g, 0, jnp.where(b1 <= g, 1, 0)))
    return xhi, yhi


def spread_centres(tiles, nt, ry, half, groups, stride, slot_ref, cent_row, packed, cen, dens, meta):
    width = 2 * half
    sub = iota((SUB, width), 0).astype(jnp.float32)
    lean = jnp.where(iota((SUB, width), 1) >= half, 0.5 * SLIDES[1], -0.5 * SLIDES[1])

    def step(r, carry):
        slot = slot_ref[r]
        rows = [cent_row[r, c] for c in range(3)]
        x, t = r // nt, r % nt
        for k in (0, 1):
            code = group_code(packed, r, k, half)
            for g in range(groups):
                i = (2 * r + k) * stride + g
                xhi, yhi = group_place(code, g)
                meta[i] = (x + xhi) * (ry + 1) + 2 * t + k + yhi
                sign = jnp.where(yhi == k, -1.0, 1.0)
                pick = slot == sub + float(k * width + g * SUB)
                p = []
                for c in range(3):
                    column = jnp.sum(jnp.where(pick, rows[c], 0.0), axis=1, keepdims=True)
                    wide = jnp.broadcast_to(column, (SUB, width))
                    if c == 1:
                        wide = wide - (0.5 * SLIDES[1] + sign * lean)
                    cen[i, c] = wide
                    dens[i, c] = wide + wide
                    p.append(wide)
                flat = (REACH - p[1] * p[1]) - p[2] * p[2]
                next_x = p[0] - SLIDES[0]
                dens[i, 3] = flat - p[0] * p[0]
                dens[i, 4] = flat - next_x * next_x
        return carry

    lax.fori_loop(0, tiles, step, 0, unroll=2)


def pair_row(rows, p, half):
    if p % 2:
        return rows[(p + 1) // 2]
    low = iota((1, 2 * half), 1) < half
    return jnp.where(low, rows[p // 2 + 1], rows[p // 2])


def build_pairs(s, first, last, ry, half, shifts, ext, pairs):
    def step(x, carry):
        rows = [[ext[s, x, t, c] for t in range(ry // 2 + 2)] for c in range(3)]
        for p in range(ry + 1):
            at = x * (ry + 1) + p
            qx, qy, qz = (pair_row(rows[c], p, half) for c in range(3))
            pairs[s, at, 0], pairs[s, at, 1] = qx, qy
            flat = qx * qx + qy * qy
            for k, shift in enumerate(shifts):
                q = qz if shift is None else qz + shift
                pairs[s, at, 2 + 2 * k] = q
                pairs[s, at, 3 + 2 * k] = -(flat + q * q)
        return carry

    lax.fori_loop(first, last, step, 0, unroll=2 if (last - first) % 2 == 0 else 1)


def build_slopes(s, cols, ry, half, ext, pairs):
    def step(x, carry):
        rows = [ext[s, x, t, 0] for t in range(ry // 2 + 2)]
        for p in range(ry + 1):
            pairs[s, x * (ry + 1) + p, 0] = pair_row(rows, p, half)
        return carry

    lax.fori_loop(0, cols, step, 0, unroll=2)


def density_layer(
    sides, first, slot, offsets, rx, groups, stride, ry, meta, pairs, table, vs, rho
):
    def run(x_cell):
        def step(j, carry):
            for g in range(groups):
                i = (x_cell * ry + j) * stride + g
                base = meta[i]
                x, y, w = table[i, 0], table[i, 1], table[i, 2]
                total = None if first else rho[i]
                for b in sides[x_cell]:
                    at = base + b * (ry + 1)
                    qx, qy = pairs[slot, at, 0], pairs[slot, at, 1]
                    xb = x - 2.0 * SLIDES[0] if b else x
                    flat = (table[i, 3 + b] + xb * qx) + y * qy
                    for k, z in enumerate(offsets):
                        qz, cq = pairs[slot, at, 2 + 2 * k], pairs[slot, at, 3 + 2 * k]
                        v = jnp.maximum(flat + (cq + w * qz), 0.0)
                        vs[i, z, b] = v
                        part = jnp.exp2(v) * (v * v)
                        total = part if total is None else total + part
                rho[i] = jnp.zeros_like(x) if total is None else total
            return carry

        return step

    for x_cell in range(rx):
        if sides[x_cell] or first:
            lax.fori_loop(0, ry, run(x_cell), 0, unroll=2)


def slope_pass(tiles, nt, half, groups, stride, slot_ref, rho, cs, root_ref, sown, sext, home):
    width = 2 * half
    sub = iota((SUB, width), 0).astype(jnp.float32)

    def step(r, carry):
        slot = slot_ref[r]
        value = jnp.zeros((SUB, width), jnp.float32)
        for k in (0, 1):
            for g in range(groups):
                i = (2 * r + k) * stride + g
                one_rho = jnp.sum(rho[i], axis=1, keepdims=True) * G1
                value = value + jnp.where(
                    slot == sub + float(k * width + g * SUB), one_rho, 0.0
                )
                one_rho = jnp.broadcast_to(one_rho, (SUB, width))
                cs[i] = (-0.5 * SIGMA) * lax.rsqrt(jnp.maximum(one_rho, 0.5))
        one_rho = jnp.sum(value, axis=0, keepdims=True)
        root = jnp.sqrt(jnp.where(slot >= 0.0, one_rho, 1.0))
        root_ref[r] = root
        row = (-0.5 * SIGMA) / root
        x, t = r // nt, r % nt
        sown[x, t, 0] = row
        sext[home, x + 1, t + 1, 0] = row
        return carry

    lax.fori_loop(0, tiles, step, 0, unroll=4)


def pair_terms(v):
    g = jnp.exp2(v) * ((v + A) * v)
    w = v * jnp.exp2(v * (8.0 / 3.0))
    return g, w * (v + B), w * v


def pair_sums(nz, spots, ry, i, base, pairs, cen, vs):
    x, y, w = cen[i, 0], cen[i, 1], cen[i, 2]
    for slot, b in spots:
        at = base + b * (ry + 1)
        dx = (x - SLIDES[0] if b else x) - pairs[slot, at, 0]
        dy = y - pairs[slot, at, 1]
        dens = pair = phi = dens_z = pair_z = 0.0
        for k, a in enumerate(offsets_of(nz, slot)):
            dz = w - pairs[slot, at, 2 + 2 * k]
            d, p, f = pair_terms(vs[i, a + DEPTH, b])
            dens, pair, phi = dens + d, pair + p, phi + f
            dens_z, pair_z = dens_z + d * dz, pair_z + p * dz
        yield slot, b, (dens * dx, dens * dy, dens_z), (pair * dx, pair * dy, pair_z, phi)


def pair_pass(
    nz, spots, first, rx, stride, ry, width, meta, pairs, cen, vs, gd, acc_ref
):
    def run(x_cell):
        def step(j, carry):
            cell = x_cell * ry + j
            for g in range(STATIC):
                i = cell * stride + g
                if first:
                    acc = [jnp.zeros((SUB, width), jnp.float32)] * 4
                else:
                    acc = [acc_ref[i, c] for c in range(4)]
                sums = pair_sums(nz, spots[x_cell], ry, i, meta[i], pairs, cen, vs)
                for slot, b, dens, pair in sums:
                    for c in range(3):
                        gd[cell * STATIC + g, slot, b, c] = dens[c]
                    acc = [total + part for total, part in zip(acc, pair)]
                for c in range(4):
                    acc_ref[i, c] = acc[c]
            return carry

        return step

    for x_cell in range(rx):
        if spots[x_cell] or first:
            lax.fori_loop(0, ry, run(x_cell), 0)


def slope_force(
    layers, cells, stride, ry, half, meta, spairs, cs, gd, acc_ref, slot_ref=None, values=None
):
    width = 2 * half
    sub = iota((SUB, width), 0).astype(jnp.float32)

    def step(cell, carry):
        if values is not None:
            marks = slot_ref[cell // 2] - (cell % 2 * width).astype(jnp.float32)
            found = [jnp.zeros((SUB, width), jnp.float32)] * 4
        for g in range(STATIC):
            i = cell * stride + g
            base, sp = meta[i], cs[i]
            acc = [acc_ref[i, c] for c in range(3)]
            for slot in layers:
                for b in (0, 1):
                    f = sp + spairs[slot, base + b * (ry + 1), 0]
                    for c in range(3):
                        acc[c] = acc[c] + f * gd[cell * STATIC + g, slot, b, c]
            if values is None:
                for c in range(3):
                    acc_ref[i, c] = acc[c]
                continue
            pick = marks == sub + float(g * SUB)
            for c, part in enumerate(acc + [acc_ref[i, 3]]):
                part = jnp.sum(part, axis=1, keepdims=True)
                found[c] = found[c] + jnp.where(pick, part, 0.0)
        if values is not None:
            for c in range(4):
                values[cell, c] = found[c]
        return carry

    lax.fori_loop(0, cells, step, 0, unroll=1 if values is None else 8)


def step_kernel(
    sizes, rx, nt, half, count_hbm, pos_hbm, slot_ref, packed, cen, pairs, vs, cs, root_ref,
    spairs, values, count_ref, pos_ref, own, ext, raw, cent_row, meta, rho, sown, sext, gd,
    acc_ref, table, load, send, recv, send2, recv2,
):
    loads = [
        pltpu.make_async_copy(count_hbm, count_ref, load.at[0]),
        pltpu.make_async_copy(pos_hbm, pos_ref, load.at[1]),
    ]
    for copy in loads:
        copy.start()
    barrier, arrivals = enter(sizes)
    ry, tiles, cells = 2 * nt, rx * nt, 2 * rx * nt
    width = 2 * half
    kept, slots = layer_slots(sizes[0])
    home = slots[DEPTH]
    groups = group_count(half)
    stride = group_stride(half)
    order = arrival_order(sizes[0])
    for copy in loads:
        copy.wait()
    load_rows(rx, nt, half, home, count_ref, pos_ref, own, ext, raw)
    assign_slots(tiles, half, raw, slot_ref, cent_row, packed)
    spread_centres(tiles, nt, ry, half, groups, stride, slot_ref, cent_row, packed, cen, table, meta)
    pl.semaphore_wait(barrier, arrivals)
    where = (sizes, rx, nt, own, ext, send, recv)
    swhere = (sizes, rx, nt, sown, sext, send2, recv2)
    start_copies(*where)

    def arrive(e, place):
        slot, known, _ = order[e]
        wait_layer(*place, slot, 1 if known is None else -known)

    def shifts_of(e):
        _, known, offsets = order[e]
        if known is None:
            return [offsets[0][0].astype(jnp.float32) * SLIDES[2]]
        return [a * SLIDES[2] if a else None for a, _ in offsets]

    def density(sides, first, e):
        slot, _, offsets = order[e]
        zs = [z for _, z in offsets]
        density_layer(
            sides, first, slot, zs, rx, groups, stride, ry, meta, pairs, table, vs, rho
        )

    def pairwise(spots, first):
        pair_pass(
            sizes[0], spots, first, rx, stride, ry, width, meta, pairs, cen, vs, gd, acc_ref
        )

    def pair_home(sides, first):
        pairwise([[(home, b) for b in side] for side in sides], first)

    both = [(0, 1)] * rx
    inner = [tuple(b for b in (0, 1) if 1 <= x + b and x + b < rx) for x in range(rx)]
    outer = [tuple(b for b in (0, 1) if b not in inner[x]) for x in range(rx)]
    wait_layer(*where, home, 0, (0,))
    build_pairs(home, 1, rx + 1, ry, half, [None], ext, pairs)
    density(inner, True, 0)
    wait_layer(*where, home, 0, (-1, 1))
    build_pairs(home, 0, 1, ry, half, [None], ext, pairs)
    build_pairs(home, rx + 1, rx + 2, ry, half, [None], ext, pairs)
    density(outer, False, 0)
    pair_home(inner, True)

    def take(e):
        arrive(e, where)
        build_pairs(order[e][0], 0, rx + 2, ry, half, shifts_of(e), ext, pairs)
        density(both, False, e)

    last = len(order) - 1
    if sizes[0] < 4:
        for e in range(1, len(order)):
            take(e)
        pair_home(outer, False)
    else:
        _, middle = nearest(sizes[0])
        take(1)
        pl.when(middle)(lambda: take(last))
        for e in range(2, last):
            take(e)
        pl.when(jnp.logical_not(middle))(lambda: take(last))
    slope_pass(tiles, nt, half, groups, stride, slot_ref, rho, cs, root_ref, sown, sext, home)
    start_copies(*swhere)
    pair_home(outer, False)
    away = [(s, b) for s in range(len(kept)) if s != home for b in (0, 1)]
    pairwise([away] * rx, False)
    for chunk in [(0, 1)] + [(e,) for e in range(2, len(order))]:
        chunk = [e for e in chunk if e < len(order)]
        for e in chunk:
            arrive(e, swhere)
            build_slopes(order[e][0], rx + 2, ry, half, sext, spairs)
        layers = [order[e][0] for e in chunk]
        final = (slot_ref, values) if chunk[-1] == len(order) - 1 else ()
        slope_force(layers, cells, stride, ry, half, meta, spairs, cs, gd, acc_ref, *final)
    wait_sends(*where)
    wait_sends(*swhere)


def finish_kernel(
    nz, rx, nt, half, slot_ref, packed, cen, pairs, vs, cs, root_ref, spairs, values,
    force_ref, energy_ref, codes, sums,
):
    width, ry, tiles = 2 * half, 2 * nt, rx * nt
    stride = group_stride(half)
    sub = iota((SUB, width), 0).astype(jnp.float32)
    spots = [(s, b) for s in range(len(layer_slots(nz)[0])) for b in (0, 1)]
    for r in range(tiles):
        for k in (0, 1):
            codes[2 * r + k] = group_code(packed, r, k, half)

    def rest(cell, carry):
        r, k = cell // 2, cell % 2
        x, j = r // nt, 2 * (r % nt) + k
        code = codes[cell]

        def group(g, carry):
            i = cell * stride + g
            sp = cs[i]
            xhi, yhi = group_place(code, g)
            base = (x + xhi) * (ry + 1) + j + yhi
            acc = [0.0] * 4
            for slot, b, dens, pair in pair_sums(nz, spots, ry, i, base, pairs, cen, vs):
                f = sp + spairs[slot, base + b * (ry + 1), 0]
                for c in range(3):
                    acc[c] = acc[c] + f * dens[c] + pair[c]
                acc[3] = acc[3] + pair[3]
            pick = slot_ref[r] == sub + (k * width + g * SUB).astype(jnp.float32)
            parts = [jnp.sum(part, axis=1, keepdims=True) for part in acc]
            return tuple(
                total + jnp.where(pick, part, 0.0) for total, part in zip(carry, parts)
            )

        start = tuple(values[cell, c] for c in range(4))
        done = lax.fori_loop(STATIC, code >> 12, group, start)
        for c in range(4):
            sums[cell, c] = done[c]
        return carry

    lax.fori_loop(0, 2 * tiles, rest, 0)

    for x in range(rx):
        for t in range(nt):
            r = x * nt + t
            for c in range(4):
                value = jnp.sum(sums[2 * r, c] + sums[2 * r + 1, c], axis=0, keepdims=True)
                if c < 3:
                    value = value * (4.0 / 3.0 * G2 / SCALE)
                else:
                    value = value * G2 - 1.0 - root_ref[r]
                value = jnp.where(slot_ref[r] >= 0.0, value, 0.0)
                for k in (0, 1):
                    part = value[:, k * half : (k + 1) * half]
                    if c < 3:
                        force_ref[c, 0, x, 2 * t + k : 2 * t + k + 1, :] = part
                    else:
                        energy_ref[0, x, 2 * t + k : 2 * t + k + 1, :] = part


def group_stride(half):
    return group_count(half)


def body(positions, counts):
    rx, ry, half = positions.shape[2:]
    nt, width = ry // 2, 2 * half
    f32 = jnp.float32
    sizes = tuple(lax.axis_size(axis) for axis in AXES)
    kept, _ = layer_slots(sizes[0])
    layers, tiles, cells = len(kept), rx * nt, rx * ry
    total = cells * group_stride(half)
    rows = (rx + 2) * (ry + 1)
    channels = 2 + 2 * max(len(offsets_of(sizes[0], s)) for s in range(layers))

    def vmem(*dims):
        return pltpu.VMEM(dims, f32)

    passed = (
            vmem(tiles, 1, width),
            vmem(tiles, 1, width),
            vmem(total, 3, SUB, width),
            vmem(layers, rows, channels, 1, width),
            vmem(total, LAYERS, 2, SUB, width),
            vmem(total, SUB, width),
            vmem(tiles, 1, width),
            vmem(layers, rows, 1, 1, width),
            vmem(cells, 4, SUB, width),
    )
    held = sum(4 * math.prod(ref.shape) for ref in passed)
    shared = pl.pallas_call(
        functools.partial(step_kernel, sizes, rx, nt, half),
        out_shape=passed,
        in_specs=[HBM, HBM],
        out_specs=(VMEM,) * len(passed),
        scratch_shapes=[
            pltpu.SMEM(counts.shape, jnp.int32),
            vmem(*positions.shape),
            vmem(rx, nt, 3, 1, width),
            vmem(layers, rx + 2, nt + 2, 3, 1, width),
            vmem(3, tiles, width),
            vmem(tiles, 3, 1, width),
            pltpu.SMEM((total,), jnp.int32),
            vmem(total, SUB, width),
            vmem(rx, nt, 1, 1, width),
            vmem(layers, rx + 2, nt + 2, 1, 1, width),
            vmem(cells * STATIC, layers, 2, 3, SUB, width),
            vmem(total, 4, SUB, width),
            vmem(total, 5, SUB, width),
            pltpu.SemaphoreType.DMA((2,)),
        ]
        + [pltpu.SemaphoreType.DMA((layers, 9))] * 4,
        compiler_params=pltpu.CompilerParams(
            collective_id=0, has_side_effects=True, vmem_limit_bytes=VMEM_BYTES - held - SPARE
        ),
        name="step",
    )(counts, positions)
    return pl.pallas_call(
        functools.partial(finish_kernel, sizes[0], rx, nt, half),
        out_shape=(
            jax.ShapeDtypeStruct((3, 1, rx, ry, half), f32),
            jax.ShapeDtypeStruct((1, rx, ry, half), f32),
        ),
        in_specs=[VMEM] * len(passed),
        out_specs=(VMEM, VMEM),
        scratch_shapes=[pltpu.SMEM((cells,), jnp.int32), vmem(cells, 4, SUB, width)],
        compiler_params=pltpu.CompilerParams(vmem_limit_bytes=24 * 2**20),
        name="finish",
    )(*shared)


def solution(mesh):
    return jax.shard_map(
        body,
        mesh=mesh,
        in_specs=(P(None, "gz", "gx", "gy", None), P("gz", "gx", "gy")),
        out_specs=(P(None, "gz", "gx", "gy", None), P("gz", "gx", "gy", None)),
        check_vma=False,
    )
```

```python
import functools
import math

import jax
import jax.numpy as jnp
from jax import lax
from jax.experimental import pallas as pl
from jax.experimental.pallas import tpu as pltpu
from jax.sharding import PartitionSpec as P

CUT = 4.95
SIDES = (12.0, 12.0, 2.5)
FAR = 1024.0
LOG2E = math.log2(math.e)
SCALE = math.sqrt(LOG2E / 8.0)
REACH = CUT * CUT * LOG2E / 8.0
SPLIT = 0.5
SLIDES = tuple(side * SCALE for side in SIDES)
A = 2.0 * LOG2E
B = 0.75 * LOG2E
G1 = 2.0 ** (-REACH) / REACH**2
G2 = 2.0 ** (-REACH * 8.0 / 3.0) / REACH**2
SIGMA = (3.0 / 16.0) * G1 / G2
CLASSES = 4
SUB = 8
STATIC = 8
VMEM_BYTES = 67_043_328
SPARE = 16384
DEPTH = 2
LAYERS = 2 * DEPTH + 1
VMEM = pl.BlockSpec(memory_space=pltpu.VMEM)
HBM = pl.BlockSpec(memory_space=pltpu.HBM)


AXES = ("gz", "gx", "gy")


def layer_slots(nz):
    kept = []
    for a in range(-DEPTH, DEPTH + 1):
        if all((a - k) % nz for k in kept):
            kept.append(a)
    slot = [
        next(i for i, k in enumerate(kept) if (a - k) % nz == 0)
        for a in range(-DEPTH, DEPTH + 1)
    ]
    return kept, slot


def displacements(sizes):
    kept, _ = layer_slots(sizes[0])
    copies, others = [], []
    for s, a in enumerate(kept):
        for b in (-1, 0, 1):
            for c in (-1, 0, 1):
                if (a, b, c) == (0, 0, 0):
                    continue
                step = tuple(-o % n for o, n in zip((a, b, c), sizes))
                copies.append((s, b, c, step))
                if any(step) and step not in others:
                    others.append(step)
    return copies, others


def device(step, sizes):
    return {
        axis: lax.rem(lax.axis_index(axis) + d + n, n)
        for axis, d, n in zip(AXES, step, sizes)
    }


def enter(sizes):
    _, others = displacements(sizes)
    barrier = pltpu.get_barrier_semaphore()
    for step in others:
        pl.semaphore_signal(
            barrier,
            inc=1,
            device_id=device(step, sizes),
            device_id_type=pl.DeviceIdType.MESH,
        )
    return barrier, len(others)


def edge(offset, length):
    if offset == 0:
        return pl.ds(0, length), pl.ds(1, length)
    if offset < 0:
        return pl.ds(length - 1, 1), pl.ds(0, 1)
    return pl.ds(0, 1), pl.ds(length + 1, 1)


def link(sizes, rx, nt, own, ext, send, recv, slot, b, c, step):
    (sx, dx), (st, dt) = edge(b, rx), edge(c, nt)
    source, target = own.at[sx, st], ext.at[slot, dx, dt]
    j = 3 * (b + 1) + c + 1
    if step is None:
        return pltpu.make_async_copy(source, target, recv.at[slot, j])
    return pltpu.make_async_remote_copy(
        src_ref=source,
        dst_ref=target,
        send_sem=send.at[slot, j],
        recv_sem=recv.at[slot, j],
        device_id=device(step, sizes),
        device_id_type=pl.DeviceIdType.MESH,
    )


def layer_links(sizes, rx, nt, own, ext, send, recv, slot, dz, sides=(-1, 0, 1)):
    found = []
    for b in sides:
        for c in (-1, 0, 1):
            step = (dz, -b, -c)
            if isinstance(dz, int):
                step = tuple(d % n for d, n in zip(step, sizes))
                if (dz, b, c) == (0, 0, 0):
                    continue
                if not any(step):
                    step = None
            copy = link(sizes, rx, nt, own, ext, send, recv, slot, b, c, step)
            found.append((copy, step is not None))
    return found


def start_layer(*where):
    for copy, _ in layer_links(*where):
        copy.start()


def wait_layer(*where):
    for copy, remote in layer_links(*where):
        if remote:
            copy.wait_recv()
        else:
            copy.wait()


def start_copies(sizes, rx, nt, own, ext, send, recv):
    nz = sizes[0]
    place = (sizes, rx, nt, own, ext, send, recv)
    kept, slots = layer_slots(nz)
    start_layer(*place, slots[DEPTH], 0)
    if nz < 4:
        for slot, a in enumerate(kept):
            if a:
                start_layer(*place, slot, -a)
        return
    near, middle = nearest(nz)

    def start_far():
        start_layer(*place, DEPTH + near, -near)

    start_layer(*place, DEPTH - near, near)
    pl.when(middle)(start_far)
    for slot in sorted({slots[0], slots[2 * DEPTH]}):
        start_layer(*place, slot, -kept[slot])
    pl.when(jnp.logical_not(middle))(start_far)


def wait_sends(sizes, rx, nt, own, ext, send, recv):
    for slot, a in enumerate(layer_slots(sizes[0])[0]):
        for copy, remote in layer_links(sizes, rx, nt, own, ext, send, recv, slot, -a):
            if remote:
                copy.wait_send()


def nearest(nz):
    z = lax.axis_index("gz")
    return jnp.where(lax.rem(z, 2) == 0, 1, -1), (z != 0) & (z != nz - 1)


def offsets_of(nz, slot):
    return [a for a in range(-DEPTH, DEPTH + 1) if layer_slots(nz)[1][a + DEPTH] == slot]


def arrival_order(nz):
    kept, slots = layer_slots(nz)
    home = slots[DEPTH]
    if nz < 4:
        rest = [s for s in range(len(kept)) if s != home]
        return [(s, kept[s], [(a, a + DEPTH) for a in offsets_of(nz, s)]) for s in [home] + rest]
    near, _ = nearest(nz)
    order = [(home, 0, [(0, DEPTH)]), (near + DEPTH, None, [(near, near + DEPTH)])]
    for s in sorted({slots[0], slots[2 * DEPTH]}):
        order.append((s, kept[s], [(a, a + DEPTH) for a in offsets_of(nz, s)]))
    order.append((DEPTH - near, None, [(-near, DEPTH - near)]))
    return order


def iota(shape, dim):
    return lax.broadcasted_iota(jnp.int32, shape, dim)


def group_count(half):
    return (half + CLASSES * (SUB - 1)) // SUB


def load_rows(rx, nt, half, home, count_ref, pos_ref, own, ext, raw):
    lane = iota((1, 2 * half), 1)
    for x in range(rx):
        for t in range(nt):
            n0, n1 = count_ref[0, x, 2 * t], count_ref[0, x, 2 * t + 1]
            occupied = jnp.where(lane < half, lane - n0, lane - half - n1) < 0
            for c in range(3):
                rows = [pos_ref[c, 0, x, 2 * t + k : 2 * t + k + 1, :] for k in (0, 1)]
                row = jnp.concatenate(rows, axis=1)
                raw[c, pl.ds(x * nt + t, 1)] = jnp.where(occupied, row, FAR)
                row = jnp.where(occupied, row * SLIDES[c], FAR)
                own[x, t, c] = row
                ext[home, x + 1, t + 1, c] = row


def assign_slots(tiles, half, raw, slot_ref, cent_row, packed):
    width = 2 * half
    u, v, w = raw[0], raw[1], raw[2]
    here = u < 0.5 * FAR
    xhi, yhi = u >= SPLIT, v >= SPLIT
    masks = [
        here & ~xhi & ~yhi,
        here & ~xhi & yhi,
        here & xhi & ~yhi,
        here & xhi & yhi,
    ]
    ones = [jnp.where(m, 1.0, 0.0) for m in masks]
    i, j = iota((width, width), 0), iota((width, width), 1)
    same = i // half == j // half
    before = jnp.where(same & (i < j), 1.0, 0.0)
    whole = jnp.where(same, 1.0, 0.0)
    stacked = jnp.concatenate(ones, axis=0)
    ranks = jnp.dot(stacked, before, preferred_element_type=jnp.float32)
    totals = jnp.dot(stacked, whole, preferred_element_type=jnp.float32)
    upper = iota((tiles, width), 1) >= half
    slot = jnp.where(here, jnp.where(upper, float(width), 0.0), -2.0 * width)
    ends = jnp.zeros((tiles, width), jnp.float32)
    pack = jnp.zeros((tiles, width), jnp.float32)
    for k in range(CLASSES):
        rank, total = ranks[k * tiles : (k + 1) * tiles], totals[k * tiles : (k + 1) * tiles]
        slot = slot + ones[k] * (ends * SUB + rank)
        ends = ends + jnp.floor((total + (SUB - 1)) * (1.0 / SUB))
        pack = pack + ends * float(16**k)
    px = u * SLIDES[0] + jnp.where(xhi, 0.0, SLIDES[0])
    py = v * SLIDES[1] + jnp.where(yhi, 0.0, SLIDES[1])
    pz = w * SLIDES[2]
    for r in range(tiles):
        slot_ref[r] = slot[r : r + 1]
        packed[r] = pack[r : r + 1]
        for c, p in enumerate((px, py, pz)):
            cent_row[r, c] = p[r : r + 1]


def group_code(packed, r, k, half):
    lane = iota((1, 2 * half), 1)
    return jnp.sum(jnp.where(lane == k * half, packed[r], 0.0)).astype(jnp.int32)


def group_place(code, g):
    b1, b2, b3 = code & 15, (code >> 4) & 15, (code >> 8) & 15
    xhi = jnp.where(b2 <= g, 1, 0)
    yhi = jnp.where(b3 <= g, 1, jnp.where(b2 <= g, 0, jnp.where(b1 <= g, 1, 0)))
    return xhi, yhi


def spread_centres(tiles, nt, ry, half, groups, stride, slot_ref, cent_row, packed, cen, dens, meta):
    width = 2 * half
    sub = iota((SUB, width), 0).astype(jnp.float32)
    lean = jnp.where(iota((SUB, width), 1) >= half, 0.5 * SLIDES[1], -0.5 * SLIDES[1])

    def step(r, carry):
        slot = slot_ref[r]
        rows = [cent_row[r, c] for c in range(3)]
        x, t = r // nt, r % nt
        for k in (0, 1):
            code = group_code(packed, r, k, half)
            for g in range(groups):
                i = (2 * r + k) * stride + g
                xhi, yhi = group_place(code, g)
                meta[i] = (x + xhi) * (ry + 1) + 2 * t + k + yhi
                sign = jnp.where(yhi == k, -1.0, 1.0)
                pick = slot == sub + float(k * width + g * SUB)
                p = []
                for c in range(3):
                    column = jnp.sum(jnp.where(pick, rows[c], 0.0), axis=1, keepdims=True)
                    wide = jnp.broadcast_to(column, (SUB, width))
                    if c == 1:
                        wide = wide - (0.5 * SLIDES[1] + sign * lean)
                    cen[i, c] = wide
                    dens[i, c] = wide + wide
                    p.append(wide)
                flat = (REACH - p[1] * p[1]) - p[2] * p[2]
                next_x = p[0] - SLIDES[0]
                dens[i, 3] = flat - p[0] * p[0]
                dens[i, 4] = flat - next_x * next_x
        return carry

    lax.fori_loop(0, tiles, step, 0, unroll=2)


def pair_row(rows, p, half):
    if p % 2:
        return rows[(p + 1) // 2]
    low = iota((1, 2 * half), 1) < half
    return jnp.where(low, rows[p // 2 + 1], rows[p // 2])


def build_pairs(s, first, last, ry, half, shifts, ext, pairs):
    def step(x, carry):
        rows = [[ext[s, x, t, c] for t in range(ry // 2 + 2)] for c in range(3)]
        for p in range(ry + 1):
            at = x * (ry + 1) + p
            qx, qy, qz = (pair_row(rows[c], p, half) for c in range(3))
            pairs[s, at, 0], pairs[s, at, 1] = qx, qy
            flat = qx * qx + qy * qy
            for k, shift in enumerate(shifts):
                q = qz if shift is None else qz + shift
                pairs[s, at, 2 + 2 * k] = q
                pairs[s, at, 3 + 2 * k] = -(flat + q * q)
        return carry

    lax.fori_loop(first, last, step, 0, unroll=2 if (last - first) % 2 == 0 else 1)


def build_slopes(s, cols, ry, half, ext, pairs):
    def step(x, carry):
        rows = [ext[s, x, t, 0] for t in range(ry // 2 + 2)]
        for p in range(ry + 1):
            pairs[s, x * (ry + 1) + p, 0] = pair_row(rows, p, half)
        return carry

    lax.fori_loop(0, cols, step, 0, unroll=4)


def density_layer(
    sides, first, slot, offsets, rx, groups, stride, ry, meta, pairs, table, vs, rho
):
    def run(x_cell):
        def step(j, carry):
            for g in range(groups):
                i = (x_cell * ry + j) * stride + g
                base = meta[i]
                x, y, w = table[i, 0], table[i, 1], table[i, 2]
                total = None if first else rho[i]
                for b in sides[x_cell]:
                    at = base + b * (ry + 1)
                    qx, qy = pairs[slot, at, 0], pairs[slot, at, 1]
                    xb = x - 2.0 * SLIDES[0] if b else x
                    flat = (table[i, 3 + b] + xb * qx) + y * qy
                    for k, z in enumerate(offsets):
                        qz, cq = pairs[slot, at, 2 + 2 * k], pairs[slot, at, 3 + 2 * k]
                        v = jnp.maximum(flat + (cq + w * qz), 0.0)
                        vs[i, z, b] = v
                        part = jnp.exp2(v) * (v * v)
                        total = part if total is None else total + part
                rho[i] = jnp.zeros_like(x) if total is None else total
            return carry

        return step

    for x_cell in range(rx):
        if sides[x_cell] or first:
            lax.fori_loop(0, ry, run(x_cell), 0, unroll=2)


def slope_pass(tiles, nt, half, groups, stride, slot_ref, rho, cs, root_ref, sown, sext, home):
    width = 2 * half
    sub = iota((SUB, width), 0).astype(jnp.float32)

    def step(r, carry):
        slot = slot_ref[r]
        value = jnp.zeros((SUB, width), jnp.float32)
        for k in (0, 1):
            for g in range(groups):
                i = (2 * r + k) * stride + g
                one_rho = jnp.sum(rho[i], axis=1, keepdims=True) * G1
                value = value + jnp.where(
                    slot == sub + float(k * width + g * SUB), one_rho, 0.0
                )
                one_rho = jnp.broadcast_to(one_rho, (SUB, width))
                cs[i] = (-0.5 * SIGMA) * lax.rsqrt(jnp.maximum(one_rho, 0.5))
        one_rho = jnp.sum(value, axis=0, keepdims=True)
        root = jnp.sqrt(jnp.where(slot >= 0.0, one_rho, 1.0))
        root_ref[r] = root
        row = (-0.5 * SIGMA) / root
        x, t = r // nt, r % nt
        sown[x, t, 0] = row
        sext[home, x + 1, t + 1, 0] = row
        return carry

    lax.fori_loop(0, tiles, step, 0, unroll=8)


def pair_terms(v):
    g = jnp.exp2(v) * ((v + A) * v)
    w = v * jnp.exp2(v * (8.0 / 3.0))
    return g, w * (v + B), w * v


def pair_sums(nz, spots, ry, i, base, pairs, cen, vs):
    x, y, w = cen[i, 0], cen[i, 1], cen[i, 2]
    for slot, b in spots:
        at = base + b * (ry + 1)
        dx = (x - SLIDES[0] if b else x) - pairs[slot, at, 0]
        dy = y - pairs[slot, at, 1]
        dens = pair = phi = dens_z = pair_z = 0.0
        for k, a in enumerate(offsets_of(nz, slot)):
            dz = w - pairs[slot, at, 2 + 2 * k]
            d, p, f = pair_terms(vs[i, a + DEPTH, b])
            dens, pair, phi = dens + d, pair + p, phi + f
            dens_z, pair_z = dens_z + d * dz, pair_z + p * dz
        yield slot, b, (dens * dx, dens * dy, dens_z), (pair * dx, pair * dy, pair_z, phi)


def pair_pass(
    nz, spots, first, rx, stride, ry, width, meta, pairs, cen, vs, gd, acc_ref
):
    def run(x_cell):
        def step(j, carry):
            cell = x_cell * ry + j
            for g in range(STATIC):
                i = cell * stride + g
                if first:
                    acc = [jnp.zeros((SUB, width), jnp.float32)] * 4
                else:
                    acc = [acc_ref[i, c] for c in range(4)]
                sums = pair_sums(nz, spots[x_cell], ry, i, meta[i], pairs, cen, vs)
                for slot, b, dens, pair in sums:
                    for c in range(3):
                        gd[cell * STATIC + g, slot, b, c] = dens[c]
                    acc = [total + part for total, part in zip(acc, pair)]
                for c in range(4):
                    acc_ref[i, c] = acc[c]
            return carry

        return step

    for x_cell in range(rx):
        if spots[x_cell] or first:
            lax.fori_loop(0, ry, run(x_cell), 0)


def slope_force(
    layers, cells, stride, ry, half, meta, spairs, cs, gd, acc_ref, slot_ref=None, values=None
):
    width = 2 * half
    sub = iota((SUB, width), 0).astype(jnp.float32)

    def step(cell, carry):
        if values is not None:
            marks = slot_ref[cell // 2] - (cell % 2 * width).astype(jnp.float32)
            found = [jnp.zeros((SUB, width), jnp.float32)] * 4
        for g in range(STATIC):
            i = cell * stride + g
            base, sp = meta[i], cs[i]
            acc = [acc_ref[i, c] for c in range(3)]
            for slot in layers:
                for b in (0, 1):
                    f = sp + spairs[slot, base + b * (ry + 1), 0]
                    for c in range(3):
                        acc[c] = acc[c] + f * gd[cell * STATIC + g, slot, b, c]
            if values is None:
                for c in range(3):
                    acc_ref[i, c] = acc[c]
                continue
            pick = marks == sub + float(g * SUB)
            for c, part in enumerate(acc + [acc_ref[i, 3]]):
                part = jnp.sum(part, axis=1, keepdims=True)
                found[c] = found[c] + jnp.where(pick, part, 0.0)
        if values is not None:
            for c in range(4):
                values[cell, c] = found[c]
        return carry

    lax.fori_loop(0, cells, step, 0, unroll=2 if values is None else 8)


def step_kernel(
    sizes, rx, nt, half, count_hbm, pos_hbm, slot_ref, packed, cen, pairs, vs, cs, root_ref,
    spairs, values, count_ref, pos_ref, own, ext, raw, cent_row, meta, rho, sown, sext, gd,
    acc_ref, table, load, send, recv, send2, recv2,
):
    loads = [
        pltpu.make_async_copy(count_hbm, count_ref, load.at[0]),
        pltpu.make_async_copy(pos_hbm, pos_ref, load.at[1]),
    ]
    for copy in loads:
        copy.start()
    barrier, arrivals = enter(sizes)
    ry, tiles, cells = 2 * nt, rx * nt, 2 * rx * nt
    width = 2 * half
    kept, slots = layer_slots(sizes[0])
    home = slots[DEPTH]
    groups = group_count(half)
    stride = group_stride(half)
    order = arrival_order(sizes[0])
    for copy in loads:
        copy.wait()
    load_rows(rx, nt, half, home, count_ref, pos_ref, own, ext, raw)
    assign_slots(tiles, half, raw, slot_ref, cent_row, packed)
    spread_centres(tiles, nt, ry, half, groups, stride, slot_ref, cent_row, packed, cen, table, meta)
    pl.semaphore_wait(barrier, arrivals)
    where = (sizes, rx, nt, own, ext, send, recv)
    swhere = (sizes, rx, nt, sown, sext, send2, recv2)
    start_copies(*where)

    def arrive(e, place):
        slot, known, _ = order[e]
        wait_layer(*place, slot, 1 if known is None else -known)

    def shifts_of(e):
        _, known, offsets = order[e]
        if known is None:
            return [offsets[0][0].astype(jnp.float32) * SLIDES[2]]
        return [a * SLIDES[2] if a else None for a, _ in offsets]

    def density(sides, first, e):
        slot, _, offsets = order[e]
        zs = [z for _, z in offsets]
        density_layer(
            sides, first, slot, zs, rx, groups, stride, ry, meta, pairs, table, vs, rho
        )

    def pairwise(spots, first):
        pair_pass(
            sizes[0], spots, first, rx, stride, ry, width, meta, pairs, cen, vs, gd, acc_ref
        )

    def pair_home(sides, first):
        pairwise([[(home, b) for b in side] for side in sides], first)

    both = [(0, 1)] * rx
    inner = [tuple(b for b in (0, 1) if 1 <= x + b and x + b < rx) for x in range(rx)]
    outer = [tuple(b for b in (0, 1) if b not in inner[x]) for x in range(rx)]
    wait_layer(*where, home, 0, (0,))
    build_pairs(home, 1, rx + 1, ry, half, [None], ext, pairs)
    density(inner, True, 0)
    wait_layer(*where, home, 0, (-1, 1))
    build_pairs(home, 0, 1, ry, half, [None], ext, pairs)
    build_pairs(home, rx + 1, rx + 2, ry, half, [None], ext, pairs)
    density(outer, False, 0)
    pair_home(inner, True)

    def take(e):
        arrive(e, where)
        build_pairs(order[e][0], 0, rx + 2, ry, half, shifts_of(e), ext, pairs)
        density(both, False, e)

    last = len(order) - 1
    if sizes[0] < 4:
        for e in range(1, len(order)):
            take(e)
        pair_home(outer, False)
    else:
        _, middle = nearest(sizes[0])
        take(1)
        pl.when(middle)(lambda: take(last))
        for e in range(2, last):
            take(e)
        pl.when(jnp.logical_not(middle))(lambda: take(last))
    slope_pass(tiles, nt, half, groups, stride, slot_ref, rho, cs, root_ref, sown, sext, home)
    start_copies(*swhere)
    pair_home(outer, False)
    away = [(s, b) for s in range(len(kept)) if s != home for b in (0, 1)]
    pairwise([away] * rx, False)
    for chunk in [(0, 1)] + [(e,) for e in range(2, len(order))]:
        chunk = [e for e in chunk if e < len(order)]
        for e in chunk:
            arrive(e, swhere)
            build_slopes(order[e][0], rx + 2, ry, half, sext, spairs)
        layers = [order[e][0] for e in chunk]
        final = (slot_ref, values) if chunk[-1] == len(order) - 1 else ()
        slope_force(layers, cells, stride, ry, half, meta, spairs, cs, gd, acc_ref, *final)
    wait_sends(*where)
    wait_sends(*swhere)


def finish_kernel(
    nz, rx, nt, half, slot_ref, packed, cen, pairs, vs, cs, root_ref, spairs, values,
    force_ref, energy_ref, codes, sums,
):
    width, ry, tiles = 2 * half, 2 * nt, rx * nt
    stride = group_stride(half)
    sub = iota((SUB, width), 0).astype(jnp.float32)
    spots = [(s, b) for s in range(len(layer_slots(nz)[0])) for b in (0, 1)]
    for r in range(tiles):
        for k in (0, 1):
            codes[2 * r + k] = group_code(packed, r, k, half)

    def rest(cell, carry):
        r, k = cell // 2, cell % 2
        x, j = r // nt, 2 * (r % nt) + k
        code = codes[cell]

        def group(g, carry):
            i = cell * stride + g
            sp = cs[i]
            xhi, yhi = group_place(code, g)
            base = (x + xhi) * (ry + 1) + j + yhi
            acc = [0.0] * 4
            for slot, b, dens, pair in pair_sums(nz, spots, ry, i, base, pairs, cen, vs):
                f = sp + spairs[slot, base + b * (ry + 1), 0]
                for c in range(3):
                    acc[c] = acc[c] + f * dens[c] + pair[c]
                acc[3] = acc[3] + pair[3]
            pick = slot_ref[r] == sub + (k * width + g * SUB).astype(jnp.float32)
            parts = [jnp.sum(part, axis=1, keepdims=True) for part in acc]
            return tuple(
                total + jnp.where(pick, part, 0.0) for total, part in zip(carry, parts)
            )

        start = tuple(values[cell, c] for c in range(4))
        done = lax.fori_loop(STATIC, code >> 12, group, start)
        for c in range(4):
            sums[cell, c] = done[c]
        return carry

    lax.fori_loop(0, 2 * tiles, rest, 0)

    for x in range(rx):
        for t in range(nt):
            r = x * nt + t
            for c in range(4):
                value = jnp.sum(sums[2 * r, c] + sums[2 * r + 1, c], axis=0, keepdims=True)
                if c < 3:
                    value = value * (4.0 / 3.0 * G2 / SCALE)
                else:
                    value = value * G2 - 1.0 - root_ref[r]
                value = jnp.where(slot_ref[r] >= 0.0, value, 0.0)
                for k in (0, 1):
                    part = value[:, k * half : (k + 1) * half]
                    if c < 3:
                        force_ref[c, 0, x, 2 * t + k : 2 * t + k + 1, :] = part
                    else:
                        energy_ref[0, x, 2 * t + k : 2 * t + k + 1, :] = part


def group_stride(half):
    return group_count(half)


def body(positions, counts):
    rx, ry, half = positions.shape[2:]
    nt, width = ry // 2, 2 * half
    f32 = jnp.float32
    sizes = tuple(lax.axis_size(axis) for axis in AXES)
    kept, _ = layer_slots(sizes[0])
    layers, tiles, cells = len(kept), rx * nt, rx * ry
    total = cells * group_stride(half)
    rows = (rx + 2) * (ry + 1)
    channels = 2 + 2 * max(len(offsets_of(sizes[0], s)) for s in range(layers))

    def vmem(*dims):
        return pltpu.VMEM(dims, f32)

    passed = (
            vmem(tiles, 1, width),
            vmem(tiles, 1, width),
            vmem(total, 3, SUB, width),
            vmem(layers, rows, channels, 1, width),
            vmem(total, LAYERS, 2, SUB, width),
            vmem(total, SUB, width),
            vmem(tiles, 1, width),
            vmem(layers, rows, 1, 1, width),
            vmem(cells, 4, SUB, width),
    )
    held = sum(4 * math.prod(ref.shape) for ref in passed)
    shared = pl.pallas_call(
        functools.partial(step_kernel, sizes, rx, nt, half),
        out_shape=passed,
        in_specs=[HBM, HBM],
        out_specs=(VMEM,) * len(passed),
        scratch_shapes=[
            pltpu.SMEM(counts.shape, jnp.int32),
            vmem(*positions.shape),
            vmem(rx, nt, 3, 1, width),
            vmem(layers, rx + 2, nt + 2, 3, 1, width),
            vmem(3, tiles, width),
            vmem(tiles, 3, 1, width),
            pltpu.SMEM((total,), jnp.int32),
            vmem(total, SUB, width),
            vmem(rx, nt, 1, 1, width),
            vmem(layers, rx + 2, nt + 2, 1, 1, width),
            vmem(cells * STATIC, layers, 2, 3, SUB, width),
            vmem(total, 4, SUB, width),
            vmem(total, 5, SUB, width),
            pltpu.SemaphoreType.DMA((2,)),
        ]
        + [pltpu.SemaphoreType.DMA((layers, 9))] * 4,
        compiler_params=pltpu.CompilerParams(
            collective_id=0, has_side_effects=True, vmem_limit_bytes=VMEM_BYTES - held - SPARE
        ),
        name="step",
    )(counts, positions)
    return pl.pallas_call(
        functools.partial(finish_kernel, sizes[0], rx, nt, half),
        out_shape=(
            jax.ShapeDtypeStruct((3, 1, rx, ry, half), f32),
            jax.ShapeDtypeStruct((1, rx, ry, half), f32),
        ),
        in_specs=[VMEM] * len(passed),
        out_specs=(VMEM, VMEM),
        scratch_shapes=[pltpu.SMEM((cells,), jnp.int32), vmem(cells, 4, SUB, width)],
        compiler_params=pltpu.CompilerParams(vmem_limit_bytes=24 * 2**20),
        name="finish",
    )(*shared)


def solution(mesh):
    return jax.shard_map(
        body,
        mesh=mesh,
        in_specs=(P(None, "gz", "gx", "gy", None), P("gz", "gx", "gy")),
        out_specs=(P(None, "gz", "gx", "gy", None), P("gz", "gx", "gy", None)),
        check_vma=False,
    )
```
